32 devices in a mesh: leaf: 8 (over z, y), blk: 4 (over x, core).
Axes of the slice: x: 2, y: 2, z: 4, core: 2. Of those that a mesh axis runs over, the one named last changes fastest.
Arguments:
- src_pos: int32 [4, 2097152], P('blk', 'leaf'), may hold values from 0 to 8388607, as said below
- strengths: float32 [2, 4, 2097152], P(None, 'blk', 'leaf'), may hold values from -0.001953125 to 0.001953125
- tgt_pos: int32 [8388608], P(('leaf', 'blk')), may hold values from 0 to 201326591, as said below
Outputs:
- field: float32 [2, 8388608], P(None, ('leaf', 'blk'))
The draws below stay inside these ranges and needn't reach their ends.
Inputs may be any that keep to these rules, and one draw needn't show every extreme that they name: `src_pos`: row q holds 16384 runs of 128 cells; run b lies in the 128 cells from (q * 16384 + b) * 128 on. `tgt_pos`: the ticks held by index k of leaf, at every index of blk, come in 2048 runs of 128; run j lies in the 12288 ticks from (j * 8 + r) * 12288 on, where r is k with its 3 binary digits in reverse order.
All inputs are finite; a program needn't handle non-finite values.
Results may differ from the reference program's by a relative error of at most 0.0003.
Values sent between devices are 32-bit elements; how exact they have to be, the bound alone decides.
No kernel may reach another device: no remote copies, remote signals or barrier semaphores. Data moves between devices by JAX's collectives and lax.ppermute only.
A program may use at most 128 MiB of HBM per device.

```python
import math
import jax
import jax.numpy as jnp
import numpy as np
from jax import lax

R = 16
PER_BOX = 128
TGT_BOX = 128
BOX_CELLS = 128
TOP_TICKS = 201326592
LB = 2048
GROUP_SRC = 2097152
N_LEAF = 8
N_BLK = 4


def draw_src_pos(key, part):
    column_count = N_LEAF * LB * PER_BOX
    row_ids = jnp.arange(N_BLK, dtype=jnp.int32)[:, None]
    columns = jnp.arange(column_count, dtype=jnp.int32)[None, :]
    box_ids = row_ids * (N_LEAF * LB) + columns // PER_BOX
    inside = jax.random.randint(jax.random.fold_in(key, 11), (N_BLK, column_count), 0, BOX_CELLS, dtype=jnp.int32)
    return box_ids * BOX_CELLS + inside


def draw_tgt_pos(key, part):
    per_device = LB * TGT_BOX
    flat_ids = jnp.arange(N_LEAF * N_BLK * per_device, dtype=jnp.int32)
    device = flat_ids // per_device
    leaf_no = device // N_BLK
    run_no = flat_ids % per_device // TGT_BOX
    bit_count = N_LEAF.bit_length() - 1
    reversed_leaf = jnp.zeros_like(leaf_no)
    for bit_no in range(bit_count):
        reversed_leaf = reversed_leaf * 2 + leaf_no // 2 ** bit_no % 2
    box_ticks = TOP_TICKS // (LB * N_LEAF)
    box_ids = run_no * N_LEAF + reversed_leaf
    inside = jax.random.randint(jax.random.fold_in(key, 23), flat_ids.shape, 0, box_ticks, dtype=jnp.int32)
    return box_ids * box_ticks + inside


def level_of(rng, extent, cuts, low, largest):
    def one(position, shards_of):
        heights = jax.random.uniform(jax.random.fold_in(jax.random.fold_in(rng, 6), position), (shards_of,), jnp.float32, low / len(cuts), largest / len(cuts))
        return jnp.repeat(jnp.exp(heights), extent[position] // shards_of).reshape((-1,) + (1,) * (len(extent) - position - 1))

    factor_of = one(*cuts[0])
    for cut in cuts[1:]:
        factor_of = factor_of * one(*cut)
    return factor_of


def gaussian(rng, dims, scale, most, shards=(), kind=jnp.bfloat16):
    drawn = scale * jax.random.normal(rng, dims, jnp.float32)
    if shards:
        drawn = drawn * level_of(rng, dims, shards, -0.22, 0.18)
    return jnp.clip(drawn, -most, most).astype(kind)


def setup_inputs(seed: int = 0) -> dict:
    splits = jax.random.split(jax.random.key(seed), 4)
    src_pos = draw_src_pos(jax.random.fold_in(splits[3], 71), 0)
    strengths = gaussian(splits[1], (2, N_BLK, GROUP_SRC), (N_BLK * GROUP_SRC) ** -0.5, 0.001953125, ((1, 4), (2, 8)), jnp.float32)
    tgt_pos = draw_tgt_pos(jax.random.fold_in(splits[3], 71), 0)
    return {"src_pos": src_pos, "strengths": strengths, "tgt_pos": tgt_pos}


highest_accuracy = lax.Precision.HIGHEST


def node_offsets(box_cells):
    node_index = np.arange(R)
    unit_nodes = (1.0 - np.cos(np.pi * (node_index + 0.5) / R)) / 2.0
    return np.floor(box_cells * unit_nodes).astype(np.int64)


def lagrange_values(node_pos, points):
    basis_rows = []
    for row_node in range(node_pos.shape[0]):
        column = np.ones(points.shape[0])
        for other_node in range(node_pos.shape[0]):
            if other_node != row_node:
                column = column * (points - node_pos[other_node]) / (node_pos[row_node] - node_pos[other_node])
        basis_rows.append(column)
    return np.stack(basis_rows)


def turn_angle(tick_ids, cell_index_list):
    product = tick_ids * cell_index_list
    return product.astype(jnp.float32) * (2.0 * math.pi / 2.0 ** 32)


def leaf_weights(in_box, amounts):
    box_count = in_box.shape[0]
    block_size = min(box_count, 512)
    center = TOP_TICKS // 2
    leaf_nodes = node_offsets(BOX_CELLS)
    node_angles = np.pi * (np.arange(R) + 0.5) / R
    exact_nodes = np.cos(node_angles)
    at_exact = lagrange_values(2.0 * leaf_nodes / BOX_CELLS - 1.0, exact_nodes)
    cheb_at = np.stack([np.cos(degree * node_angles) for degree in range(R)])
    norm_weights = np.where(np.arange(R) == 0, 1.0, 2.0) / R
    coefficients = jnp.asarray(norm_weights[:, None] * (cheb_at @ at_exact.T), jnp.float32)

    def one_block(block_no):
        box_part = lax.dynamic_slice_in_dim(in_box, block_no * block_size, block_size, 0)
        strength_blk = lax.dynamic_slice_in_dim(amounts, block_no * block_size, block_size, 1)
        angles = turn_angle(jnp.int32(center), box_part)
        rotate_re = jnp.cos(angles)
        rotation_imaginary = jnp.sin(angles)
        source_re = rotate_re * strength_blk[0] - rotation_imaginary * strength_blk[1]
        source_im = rotation_imaginary * strength_blk[0] + rotate_re * strength_blk[1]
        scaled = box_part.astype(jnp.float32) * (2.0 / BOX_CELLS) - 1.0
        chebyshev = [jnp.ones_like(scaled), scaled]
        for degree in range(2, R):
            chebyshev.append(2.0 * scaled * chebyshev[-1] - chebyshev[-2])
        moments = jnp.einsum('nbk,xbk->xnb', jnp.stack(chebyshev), jnp.stack([source_re, source_im]), precision=highest_accuracy)
        return jnp.einsum('nt,xnb->xtb', coefficients, moments, precision=highest_accuracy)

    blocks = lax.map(one_block, jnp.arange(box_count // block_size, dtype=jnp.int32))
    mixed_nodes = jnp.transpose(blocks, (1, 2, 0, 3)).reshape(2, R, box_count)
    post_turn = turn_angle(jnp.int32(center), jnp.asarray(leaf_nodes, jnp.int32))
    post_re = jnp.cos(post_turn)[:, None]
    post_im = jnp.sin(post_turn)[:, None]
    out_re = post_re * mixed_nodes[0] + post_im * mixed_nodes[1]
    out_im = post_re * mixed_nodes[1] - post_im * mixed_nodes[0]
    return jnp.stack([out_re, out_im]).reshape(2, R, 1, box_count)


def parent_level(paired, child_ids, tree_level):
    box_a = child_ids.shape[0]
    box_e = child_ids.shape[1]
    box_s = paired.shape[3]
    child_cells = BOX_CELLS * 2 ** tree_level
    child_nodes = node_offsets(child_cells)
    parent_nodes = node_offsets(2 * child_cells)
    inner_cells = np.concatenate([child_nodes, child_nodes + child_cells])
    blend_matrix = jnp.asarray(lagrange_values(parent_nodes / (2.0 * child_cells), inner_cells / (2.0 * child_cells)).reshape(R, 2, R), jnp.float32)
    box_ticks = TOP_TICKS // 2 ** (tree_level + 1)
    centers = child_ids * box_ticks + box_ticks // 2
    pre_turn = turn_angle(centers[:, :, None], jnp.asarray(inner_cells, jnp.int32)[None, None, :]).reshape(box_a, box_e, 2, R)
    pre_re = jnp.cos(pre_turn)[..., None]
    pre_im = jnp.sin(pre_turn)[..., None]
    source = jnp.transpose(paired, (0, 2, 4, 1, 3))[:, :, None]
    rotated_real = pre_re * source[0] - pre_im * source[1]
    rotated_imaginary = pre_im * source[0] + pre_re * source[1]
    accumulated_sum = jnp.einsum('jiw,fpziwd->fjpzd', blend_matrix, jnp.stack([rotated_real, rotated_imaginary]), precision=highest_accuracy)
    post_turn = turn_angle(centers[:, :, None], jnp.asarray(parent_nodes, jnp.int32)[None, None, :])
    post_re = jnp.transpose(jnp.cos(post_turn), (2, 0, 1))[:, :, :, None]
    post_im = jnp.transpose(jnp.sin(post_turn), (2, 0, 1))[:, :, :, None]
    out_re = post_re * accumulated_sum[0] + post_im * accumulated_sum[1]
    out_im = post_re * accumulated_sum[1] - post_im * accumulated_sum[0]
    return jnp.stack([out_re, out_im]).reshape(2, R, box_a * box_e, box_s)


def tree_up(weights, tree_level, first_box):
    box_a = weights.shape[2]
    box_s = weights.shape[3]
    paired = weights.reshape(2, R, box_a, box_s // 2, 2)
    parents = first_box + jnp.arange(box_a, dtype=jnp.int32)
    child_ids = 2 * parents[:, None] + jnp.arange(2, dtype=jnp.int32)[None, :]
    return parent_level(paired, child_ids, tree_level)


def reference(src_pos, strengths, tgt_pos):
    block_count = src_pos.shape[0]
    group_boxes = src_pos.shape[1] // PER_BOX
    tree_depth = group_boxes.bit_length() - 1
    group_cells = group_boxes * BOX_CELLS
    root_list = []
    for source_blk in range(block_count):
        in_box = (src_pos[source_blk] % BOX_CELLS).reshape(group_boxes, PER_BOX)
        amounts = strengths[:, source_blk].reshape(2, group_boxes, PER_BOX)
        weights = leaf_weights(in_box, amounts)
        for tree_level in range(tree_depth):
            weights = tree_up(weights, tree_level, 0)
        root_list.append(weights.reshape(2, R, group_boxes))
    root_sets = jnp.stack(root_list)
    top_nodes = jnp.asarray(node_offsets(group_cells), jnp.int32)
    final_ticks = TOP_TICKS // group_boxes
    target_count = tgt_pos.shape[0]
    block_size = min(target_count, 65536)

    def one_block(block_no):
        ticks_blk = lax.dynamic_slice_in_dim(tgt_pos, block_no * block_size, block_size, 0)
        box_ids = ticks_blk // final_ticks
        picked = jnp.take(root_sets, box_ids, axis=3)
        angles = turn_angle(ticks_blk[None, :], top_nodes[:, None])
        phase_re = jnp.cos(angles)
        phase_im = jnp.sin(angles)
        field_re = jnp.zeros(ticks_blk.shape, jnp.float32)
        field_imaginary = jnp.zeros(ticks_blk.shape, jnp.float32)
        for source_blk in range(block_count):
            part_re = picked[source_blk, 0]
            part_im = picked[source_blk, 1]
            inner_re = jnp.sum(phase_re * part_re - phase_im * part_im, axis=0)
            inner_im = jnp.sum(phase_re * part_im + phase_im * part_re, axis=0)
            outer_turn = turn_angle(ticks_blk, jnp.int32(source_blk * group_cells))
            outer_re = jnp.cos(outer_turn)
            outer_im = jnp.sin(outer_turn)
            field_re = field_re + outer_re * inner_re - outer_im * inner_im
            field_imaginary = field_imaginary + outer_re * inner_im + outer_im * inner_re
        return jnp.stack([field_re, field_imaginary])

    blocks = lax.map(one_block, jnp.arange(target_count // block_size, dtype=jnp.int32))
    return jnp.transpose(blocks, (1, 0, 2)).reshape(2, target_count)
```

```python
import functools
import math

import jax
import jax.numpy as jnp
import numpy as np
from jax import lax
from jax.experimental import pallas as pl
from jax.experimental.pallas import tpu as pltpu
from jax.sharding import PartitionSpec as P

R = 16
PER_BOX = 128
TGT_BOX = 128
BOX_CELLS = 128
TOP_TICKS = 201326592
LANES = 128
ROWS = 2 * R
HALF = R // 2

SIN_COEFS = (4.44288292, -7.30824569, 3.60635422, -0.84611165, 0.10982452)
COS_COEFS = (1.4142135, -6.97885095, 5.73946038, -1.88355791, 0.31068803)


def node_offsets(box_cells):
    node_index = np.arange(R)
    unit_nodes = (1.0 - np.cos(np.pi * (node_index + 0.5) / R)) / 2.0
    return np.floor(box_cells * unit_nodes).astype(np.int64)


def lagrange_values(node_pos, points):
    basis_rows = []
    for row_node in range(node_pos.shape[0]):
        column = np.ones(points.shape[0])
        for other_node in range(node_pos.shape[0]):
            if other_node != row_node:
                column = (
                    column
                    * (points - node_pos[other_node])
                    / (node_pos[row_node] - node_pos[other_node])
                )
        basis_rows.append(column)
    return np.stack(basis_rows)


def turn_exp(ticks, cells):
    product = (ticks * cells) % 2**32
    return np.exp(2j * np.pi * (product / 2.0**32))


def as_real(matrix):
    return np.block([[matrix.real, -matrix.imag], [matrix.imag, matrix.real]])


def level_blocks(tree_level):
    child_cells = BOX_CELLS * 2**tree_level
    box_ticks = TOP_TICKS // 2**tree_level
    assert box_ticks // 2 * child_cells % 2**32 == 0
    child_nodes = node_offsets(child_cells)
    parent_nodes = node_offsets(2 * child_cells)
    inner_cells = np.concatenate([child_nodes, child_nodes + child_cells])
    blend = lagrange_values(
        parent_nodes / (2.0 * child_cells), inner_cells / (2.0 * child_cells)
    ).reshape(R, 2, R)
    blend = blend.astype(np.float32).astype(np.float64)
    center = box_ticks // 4
    return [
        [
            blend[:, child]
            * turn_exp((2 * half - 1) * (box_ticks // 4), child_nodes)[None, :]
            * turn_exp(center, child * child_cells)
            for child in range(2)
        ]
        for half in range(2)
    ]


def stage_matrix(first_level, order):
    count = len(order)
    size = 2**count
    levels = [level_blocks(first_level + step) for step in range(count)]
    place = [order.index(step) for step in range(count)]
    full = np.zeros((size, ROWS, size, ROWS))
    for out_block in range(size):
        for in_block in range(size):
            matrix = np.eye(R)
            for step in range(count):
                bits = (out_block >> place[step] & 1, in_block >> place[step] & 1)
                matrix = levels[step][bits[0]][bits[1]] @ matrix
            full[out_block, :, in_block, :] = as_real(matrix)
    return full


def product_basis():
    table = np.zeros((R, R))
    for high in range(4):
        for low in range(4):
            for degree in (4 * high + low, abs(4 * high - low)):
                table[4 * high + low, degree] += 0.5
    return table


def leaf_matrix():
    leaf_nodes = node_offsets(BOX_CELLS)
    node_angles = np.pi * (np.arange(R) + 0.5) / R
    at_exact = lagrange_values(2.0 * leaf_nodes / BOX_CELLS - 1.0, np.cos(node_angles))
    cheb_at = np.stack([np.cos(degree * node_angles) for degree in range(R)])
    norm_weights = np.where(np.arange(R) == 0, 1.0, 2.0) / R
    coefficients = norm_weights[:, None] * (cheb_at @ at_exact.T)
    coefficients = coefficients.astype(np.float32).astype(np.float64)
    return as_real(coefficients.T @ np.linalg.inv(product_basis()))


def field_rows():
    table = np.zeros((4, HALF, 2, R))
    for node in range(HALF):
        mirror = R - 1 - node
        table[0, node, 0, [node, mirror]] = 1.0
        table[1, node, 1, [node, mirror]] = [1.0, -1.0]
        table[2, node, 1, [node, mirror]] = 1.0
        table[3, node, 0, [node, mirror]] = [-1.0, 1.0]
    return table.reshape(ROWS, ROWS)


def split_table(matrix):
    high = matrix.astype(np.float32).astype(jnp.bfloat16)
    low = (matrix - high.astype(np.float64)).astype(np.float32).astype(jnp.bfloat16)
    return np.concatenate([high, high, low], axis=-1)


def split_value(value):
    high = value.astype(jnp.bfloat16)
    low = (value - high.astype(jnp.float32)).astype(jnp.bfloat16)
    return jnp.concatenate([high, low, high], axis=0)


def times_table(table, value):
    return jnp.dot(table, split_value(value), preferred_element_type=jnp.float32)


def polynomial(coefs, value):
    total = jnp.full_like(value, coefs[-1])
    for coef in coefs[-2::-1]:
        total = total * value + coef
    return total


def unit_circle(turns):
    rest = turns - jnp.round(turns)
    square = rest * rest
    sine = rest * polynomial(SIN_COEFS, square)
    cosine = polynomial(COS_COEFS, square)
    return 1.0 - sine * sine, sine * cosine


def reverse_bits(value, count):
    return sum((value >> bit & 1) << (count - 1 - bit) for bit in range(count))


def swap_bits(blocks, block_bit, lane_bit):
    step = 1 << lane_bit
    shape = blocks[0].shape
    upper = (lax.broadcasted_iota(jnp.int32, shape, 1) >> lane_bit & 1) == 1
    swapped = list(blocks)
    for number in range(len(blocks)):
        if not number >> block_bit & 1:
            other = number | 1 << block_bit
            low, high = blocks[number], blocks[other]
            swapped[number] = jnp.where(upper, pltpu.roll(high, step, 1), low)
            swapped[other] = jnp.where(upper, high, pltpu.roll(low, LANES - step, 1))
    return swapped


def run_stage(blocks, row_bits, table):
    count = len(blocks)
    side_bits = [bit for bit in range(count.bit_length() - 1) if bit not in row_bits]

    def number(row, side):
        return sum((row >> k & 1) << bit for k, bit in enumerate(row_bits)) + sum(
            (side >> k & 1) << bit for k, bit in enumerate(side_bits)
        )

    sides = range(2 ** len(side_bits))
    rows = range(2 ** len(row_bits))
    value = jnp.concatenate(
        [
            jnp.concatenate([blocks[number(row, side)] for row in rows], axis=0)
            for side in sides
        ],
        axis=1,
    )
    product = times_table(table, value)
    result = list(blocks)
    for side in sides:
        for row in rows:
            result[number(row, side)] = product[
                row * ROWS : (row + 1) * ROWS, side * LANES : (side + 1) * LANES
            ]
    return result


def source_kernel(pos_ref, strength_ref, t1_ref, t2_ref, t3_ref, t4_ref, out_ref, moments):
    tile_count = pos_ref.shape[0] // LANES
    center = TOP_TICKS // 2
    turn_rate = center / 2.0**32

    def one_tile(tile, carry):
        parts = [[], [], []]
        for group in range(16):
            start = tile * LANES + 8 * reverse_bits(group, 4)
            rows = pl.ds(pl.multiple_of(start, 8), 8)
            cell = (pos_ref[rows, :] & (BOX_CELLS - 1)).astype(jnp.float32)
            rot_re, rot_im = unit_circle(cell * turn_rate)
            real = strength_ref[0, rows, :]
            imag = strength_ref[1, rows, :]
            parts[0].append(cell * (2.0 / BOX_CELLS) - 1.0)
            parts[1].append(rot_re * real - rot_im * imag)
            parts[2].append(rot_im * real + rot_re * imag)
        scaled, real, imag = (jnp.concatenate(part, axis=0).T for part in parts)
        sums = [None] * ROWS
        for group in range(16):
            rows = slice(8 * group, 8 * group + 8)
            v = scaled[rows]
            t2 = 2.0 * (v * v) - 1.0
            t3 = v * (2.0 * t2 - 1.0)
            t4 = 2.0 * (t2 * t2) - 1.0
            t8 = 2.0 * (t4 * t4) - 1.0
            t12 = t4 * (2.0 * t8 - 1.0)
            for side, value in enumerate((real[rows], imag[rows])):
                for high, outer in enumerate((None, t4, t8, t12)):
                    base = value if outer is None else value * outer
                    for low, inner in enumerate((None, v, t2, t3)):
                        term = base if inner is None else base * inner
                        row = side * R + 4 * high + low
                        sums[row] = term if sums[row] is None else sums[row] + term
        for row in range(ROWS):
            moments[tile, pl.ds(row, 1), :] = jnp.sum(sums[row], axis=0, keepdims=True)
        return carry

    lax.fori_loop(0, tile_count, one_tile, 0)
    blocks = [moments[tile] for tile in range(tile_count)]
    for block_bit, lane_bit in ((0, 2), (1, 1), (2, 0)):
        blocks = swap_bits(blocks, block_bit, lane_bit)
    blocks = run_stage(blocks, (0, 1, 2), t1_ref[...])
    for block_bit, lane_bit in ((2, 6), (1, 5), (0, 4)):
        blocks = swap_bits(blocks, block_bit, lane_bit)
    blocks = run_stage(blocks, (0, 1, 2), t2_ref[...])
    for block_bit, lane_bit in ((2, 3), (1, 2), (0, 1)):
        blocks = swap_bits(blocks, block_bit, lane_bit)
    blocks = run_stage(blocks, (0, 1, 2), t3_ref[...])
    blocks = swap_bits(blocks, 2, 0)
    blocks = run_stage(blocks, (2, 3), t4_ref[...])
    for number in range(tile_count):
        place = sum((number >> bit & 1) << to for bit, to in ((0, 2), (1, 3), (2, 1), (3, 0)))
        out_ref[:, place * LANES : (place + 1) * LANES] = blocks[number]


def source_tables():
    first = stage_matrix(0, [2, 1, 0])
    first = np.einsum("abcd,de->abce", first, leaf_matrix())
    second = stage_matrix(3, [2, 1, 0])
    third = stage_matrix(6, [2, 1, 0])
    fourth = stage_matrix(9, [0, 1])
    return [
        jnp.asarray(split_table(table.reshape(len(table) * ROWS, -1)))
        for table in (first, second, third, fourth)
    ]


def join_kernel(side_ref, own_ref, partner_ref, table_ref, out_ref):
    value = jnp.concatenate([own_ref[...], partner_ref[...]], axis=0)
    out_ref[...] = times_table(table_ref[side_ref[0]], value)


def join_table(tree_level, last):
    blocks = level_blocks(tree_level)
    sides = []
    for side in range(2):
        table = np.concatenate(
            [as_real(blocks[side][side]), as_real(blocks[side][1 - side])], axis=1
        )
        sides.append(split_table(field_rows() @ table if last else table))
    return jnp.asarray(np.stack(sides))


def field_kernel(base_ref, tgt_ref, *refs, leaf_count, group_cells):
    roots, (out_ref, offsets, field) = refs[:-3], refs[-3:]
    box_count = tgt_ref.shape[0]
    tile_count = box_count // LANES
    box_ticks = TOP_TICKS // (box_count * leaf_count)
    rates = (group_cells - 1 - 2 * node_offsets(group_cells)[:HALF]) / 2.0**33
    chunk = 16

    def one_tile(tile, carry):
        ticks = tgt_ref[pl.ds(tile, LANES, stride=tile_count), :]
        box = lax.broadcasted_iota(jnp.int32, ticks.shape, 0) * tile_count + tile
        center = box * (leaf_count * box_ticks) + base_ref[0]
        offsets[...] = (ticks - center).astype(jnp.float32).T

        def one_chunk(part, inner_carry):
            rows = pl.ds(pl.multiple_of(part * chunk, chunk), chunk)
            x = offsets[rows, :]
            sums = [[None, None] for _ in roots]
            columns = pl.ds(pl.multiple_of(tile * LANES, LANES), LANES)
            for node in range(HALF):
                cosine, sine = unit_circle(x * float(rates[node]))
                for root, total in zip(roots, sums):
                    for side in range(2):
                        row = 2 * side * HALF + node
                        term = cosine * root[pl.ds(row, 1), columns]
                        term = term + sine * root[pl.ds(row + HALF, 1), columns]
                        total[side] = term if total[side] is None else total[side] + term
            mid_re, mid_im = unit_circle(x * float((group_cells - 1) / 2.0**33))
            z_re, z_im = unit_circle(x * float(group_cells / 2.0**32))
            real, imag = sums[-1]
            for total in sums[-2::-1]:
                real, imag = (
                    z_re * real - z_im * imag + total[0],
                    z_re * imag + z_im * real + total[1],
                )
            field[0, rows, :] = mid_re * real - mid_im * imag
            field[1, rows, :] = mid_re * imag + mid_im * real
            return inner_carry

        lax.fori_loop(0, TGT_BOX // chunk, one_chunk, 0)
        for side in range(2):
            rows = pl.ds(2 * tile + side, LANES, stride=2 * tile_count)
            out_ref[rows, :] = field[side].T
        return carry

    lax.fori_loop(0, tile_count, one_tile, 0)


def whole_vmem(count):
    return [pl.BlockSpec(memory_space=pltpu.VMEM)] * count


def partner_2(block, axis, apart):
    count = lax.axis_size(axis)
    route = []
    for low in range(count):
        high = low | 1 << apart
        if high != low and high < count:
            route += [(low, high), (high, low)]
    return lax.ppermute(block, axis, route)


def local(src_pos, strengths, tgt_pos):
    leaf_count = lax.axis_size("leaf")
    leaf_bits = leaf_count.bit_length() - 1
    leaf_no = lax.axis_index("leaf")
    box_count = src_pos.shape[1] // PER_BOX
    local_depth = box_count.bit_length() - 1
    assert box_count == 16 * LANES
    group_cells = box_count * leaf_count * BOX_CELLS
    box_ticks = TOP_TICKS // (box_count * leaf_count)
    offsets = node_offsets(group_cells)
    assert (offsets + offsets[::-1] == group_cells - 1).all()
    assert box_ticks // 2 * group_cells % 2**32 == 0

    weights = pl.pallas_call(
        source_kernel,
        out_shape=jax.ShapeDtypeStruct((ROWS, box_count), jnp.float32),
        in_specs=whole_vmem(6),
        out_specs=pl.BlockSpec(memory_space=pltpu.VMEM),
        scratch_shapes=[pltpu.VMEM((box_count // LANES, ROWS, LANES), jnp.float32)],
        name="sources",
    )(
        src_pos.reshape(box_count, PER_BOX),
        strengths.reshape(2, box_count, PER_BOX),
        *source_tables(),
    )

    suffix = jnp.int32(0)
    for bit_no in range(leaf_bits):
        own_side = leaf_no // 2**bit_no % 2
        partner = partner_2(weights, "leaf", bit_no)
        weights = pl.pallas_call(
            join_kernel,
            out_shape=jax.ShapeDtypeStruct(weights.shape, jnp.float32),
            in_specs=[pl.BlockSpec(memory_space=pltpu.SMEM)] + whole_vmem(3),
            out_specs=pl.BlockSpec(memory_space=pltpu.VMEM),
            name="join",
        )(
            own_side.reshape(1),
            weights,
            partner,
            join_table(local_depth + bit_no, bit_no == leaf_bits - 1),
        )
        suffix = 2 * suffix + own_side

    blk_count = lax.axis_size("blk")
    gathered = lax.all_gather(weights[:HALF * 2], "blk"), lax.all_gather(weights[HALF * 2:], "blk")
    roots = jnp.concatenate(gathered, axis=1)
    base = suffix * box_ticks + box_ticks // 2
    field = pl.pallas_call(
        functools.partial(field_kernel, leaf_count=leaf_count, group_cells=group_cells),
        out_shape=jax.ShapeDtypeStruct((2 * box_count, TGT_BOX), jnp.float32),
        in_specs=[pl.BlockSpec(memory_space=pltpu.SMEM)] + whole_vmem(1 + blk_count),
        out_specs=pl.BlockSpec(memory_space=pltpu.VMEM),
        scratch_shapes=[
            pltpu.VMEM((TGT_BOX, LANES), jnp.float32),
            pltpu.VMEM((2, TGT_BOX, LANES), jnp.float32),
        ],
        name="targets",
    )(base.reshape(1), tgt_pos.reshape(box_count, TGT_BOX), *[roots[q] for q in range(blk_count)])
    field = field.reshape(box_count, 2, TGT_BOX)
    return jnp.transpose(field, (1, 0, 2)).reshape(2, box_count * TGT_BOX)


def solution(mesh):
    return jax.shard_map(
        local,
        mesh=mesh,
        in_specs=(P("blk", "leaf"), P(None, "blk", "leaf"), P(("leaf", "blk"))),
        out_specs=P(None, ("leaf", "blk")),
        check_vma=False,
    )
```

```python
import functools
import math

import jax
import jax.numpy as jnp
import numpy as np
from jax import lax
from jax.experimental import pallas as pl
from jax.experimental.pallas import tpu as pltpu
from jax.sharding import PartitionSpec as P

R = 16
PER_BOX = 128
TGT_BOX = 128
BOX_CELLS = 128
TOP_TICKS = 201326592
LANES = 128
ROWS = 2 * R
HALF = R // 2
CHUNKS = 2
PHASE_PARTS = 4
PHASE_PLAN = (1, 1, 2)
LEAF_STEPS = 4

SIN_COEFS = (4.44288292, -7.30824569, 3.60635422, -0.84611165, 0.10982452)
COS_COEFS = (1.4142135, -6.97885095, 5.73946038, -1.88355791, 0.31068803)


def node_offsets(box_cells):
    node_index = np.arange(R)
    unit_nodes = (1.0 - np.cos(np.pi * (node_index + 0.5) / R)) / 2.0
    return np.floor(box_cells * unit_nodes).astype(np.int64)


def lagrange_values(node_pos, points):
    basis_rows = []
    for row_node in range(node_pos.shape[0]):
        column = np.ones(points.shape[0])
        for other_node in range(node_pos.shape[0]):
            if other_node != row_node:
                column = (
                    column
                    * (points - node_pos[other_node])
                    / (node_pos[row_node] - node_pos[other_node])
                )
        basis_rows.append(column)
    return np.stack(basis_rows)


def turn_exp(ticks, cells):
    product = (ticks * cells) % 2**32
    return np.exp(2j * np.pi * (product / 2.0**32))


def as_real(matrix):
    return np.block([[matrix.real, -matrix.imag], [matrix.imag, matrix.real]])


def level_blocks(tree_level):
    child_cells = BOX_CELLS * 2**tree_level
    box_ticks = TOP_TICKS // 2**tree_level
    assert box_ticks // 2 * child_cells % 2**32 == 0
    child_nodes = node_offsets(child_cells)
    parent_nodes = node_offsets(2 * child_cells)
    inner_cells = np.concatenate([child_nodes, child_nodes + child_cells])
    blend = lagrange_values(
        parent_nodes / (2.0 * child_cells), inner_cells / (2.0 * child_cells)
    ).reshape(R, 2, R)
    blend = blend.astype(np.float32).astype(np.float64)
    center = box_ticks // 4
    return [
        [
            blend[:, child]
            * turn_exp((2 * half - 1) * (box_ticks // 4), child_nodes)[None, :]
            * turn_exp(center, child * child_cells)
            for child in range(2)
        ]
        for half in range(2)
    ]


def stage_matrix(first_level, order):
    count = len(order)
    size = 2**count
    levels = [level_blocks(first_level + step) for step in range(count)]
    place = [order.index(step) for step in range(count)]
    full = np.zeros((size, ROWS, size, ROWS))
    for out_block in range(size):
        for in_block in range(size):
            matrix = np.eye(R)
            for step in range(count):
                bits = (out_block >> place[step] & 1, in_block >> place[step] & 1)
                matrix = levels[step][bits[0]][bits[1]] @ matrix
            full[out_block, :, in_block, :] = as_real(matrix)
    return full


def product_basis():
    table = np.zeros((R, R))
    for high in range(4):
        for low in range(4):
            for degree in (4 * high + low, abs(4 * high - low)):
                table[4 * high + low, degree] += 0.5
    return table


def leaf_matrix():
    leaf_nodes = node_offsets(BOX_CELLS)
    node_angles = np.pi * (np.arange(R) + 0.5) / R
    at_exact = lagrange_values(2.0 * leaf_nodes / BOX_CELLS - 1.0, np.cos(node_angles))
    cheb_at = np.stack([np.cos(degree * node_angles) for degree in range(R)])
    norm_weights = np.where(np.arange(R) == 0, 1.0, 2.0) / R
    coefficients = norm_weights[:, None] * (cheb_at @ at_exact.T)
    coefficients = coefficients.astype(np.float32).astype(np.float64)
    return as_real(coefficients.T @ np.linalg.inv(product_basis()))


def field_rows():
    table = np.zeros((4, HALF, 2, R))
    for node in range(HALF):
        mirror = R - 1 - node
        table[0, node, 0, [node, mirror]] = 1.0
        table[1, node, 1, [node, mirror]] = [1.0, -1.0]
        table[2, node, 1, [node, mirror]] = 1.0
        table[3, node, 0, [node, mirror]] = [-1.0, 1.0]
    return table.reshape(ROWS, ROWS)


def split_table(matrix):
    high = matrix.astype(np.float32).astype(jnp.bfloat16)
    low = (matrix - high.astype(np.float64)).astype(np.float32).astype(jnp.bfloat16)
    return np.concatenate([high, high, low], axis=-1)


def split_value(value):
    high = value.astype(jnp.bfloat16)
    low = (value - high.astype(jnp.float32)).astype(jnp.bfloat16)
    return jnp.concatenate([high, low, high], axis=0)


def times_table(table, value):
    return jnp.dot(table, split_value(value), preferred_element_type=jnp.float32)


def polynomial(coefs, value):
    total = jnp.full_like(value, coefs[-1])
    for coef in coefs[-2::-1]:
        total = total * value + coef
    return total


def unit_circle(turns):
    rest = turns - jnp.round(turns)
    square = rest * rest
    sine = rest * polynomial(SIN_COEFS, square)
    cosine = polynomial(COS_COEFS, square)
    return 1.0 - sine * sine, sine * cosine


def reverse_bits(value, count):
    return sum((value >> bit & 1) << (count - 1 - bit) for bit in range(count))


def swap_bits(blocks, block_bit, lane_bit):
    step = 1 << lane_bit
    shape = blocks[0].shape
    upper = (lax.broadcasted_iota(jnp.int32, shape, 1) >> lane_bit & 1) == 1
    swapped = list(blocks)
    for number in range(len(blocks)):
        if not number >> block_bit & 1:
            other = number | 1 << block_bit
            low, high = blocks[number], blocks[other]
            swapped[number] = jnp.where(upper, pltpu.roll(high, step, 1), low)
            swapped[other] = jnp.where(upper, high, pltpu.roll(low, LANES - step, 1))
    return swapped


def run_stage(blocks, row_bits, table):
    count = len(blocks)
    side_bits = [bit for bit in range(count.bit_length() - 1) if bit not in row_bits]

    def number(row, side):
        return sum((row >> k & 1) << bit for k, bit in enumerate(row_bits)) + sum(
            (side >> k & 1) << bit for k, bit in enumerate(side_bits)
        )

    sides = range(2 ** len(side_bits))
    rows = range(2 ** len(row_bits))
    value = jnp.concatenate(
        [
            jnp.concatenate([blocks[number(row, side)] for row in rows], axis=0)
            for side in sides
        ],
        axis=1,
    )
    product = times_table(table, value)
    result = list(blocks)
    for side in sides:
        for row in rows:
            result[number(row, side)] = product[
                row * ROWS : (row + 1) * ROWS, side * LANES : (side + 1) * LANES
            ]
    return result


def leaf_kernel(pos_ref, strength_ref, *refs):
    count = (len(refs) - 2) // 2
    out_ref, semaphores = refs[count], refs[-1]
    copies = [
        pltpu.make_async_copy(source, target, semaphores.at[number])
        for number, (source, target) in enumerate(zip(refs[:count], refs[count + 1 : -1]))
    ]

    @pl.when(pl.program_id(0) == 0)
    def start_copies():
        for copy in copies:
            copy.start()

    center = TOP_TICKS // 2
    turn_rate = center / 2.0**32
    tile_count = pos_ref.shape[0] // LANES
    first = pl.program_id(0) * tile_count

    def one_tile(tile, carry):
        parts = [[], [], []]
        for group in range(16):
            start = tile * LANES + 8 * reverse_bits(group, 4)
            rows = pl.ds(pl.multiple_of(start, 8), 8)
            cell = (pos_ref[rows, :] & (BOX_CELLS - 1)).astype(jnp.float32)
            rot_re, rot_im = unit_circle(cell * turn_rate)
            real = strength_ref[0, rows, :]
            imag = strength_ref[1, rows, :]
            parts[0].append(cell * (2.0 / BOX_CELLS) - 1.0)
            parts[1].append(rot_re * real - rot_im * imag)
            parts[2].append(rot_im * real + rot_re * imag)
        scaled, real, imag = (jnp.concatenate(part, axis=0).T for part in parts)
        sums = [None] * ROWS
        for group in range(16):
            rows = slice(8 * group, 8 * group + 8)
            v = scaled[rows]
            t2 = 2.0 * (v * v) - 1.0
            t3 = v * (2.0 * t2 - 1.0)
            t4 = 2.0 * (t2 * t2) - 1.0
            t8 = 2.0 * (t4 * t4) - 1.0
            t12 = t4 * (2.0 * t8 - 1.0)
            for side, value in enumerate((real[rows], imag[rows])):
                for high, outer in enumerate((None, t4, t8, t12)):
                    base = value if outer is None else value * outer
                    for low, inner in enumerate((None, v, t2, t3)):
                        term = base if inner is None else base * inner
                        row = side * R + 4 * high + low
                        sums[row] = term if sums[row] is None else sums[row] + term
        for row in range(ROWS):
            out_ref[first + tile, pl.ds(row, 1), :] = jnp.sum(sums[row], axis=0, keepdims=True)
        return carry

    lax.fori_loop(0, tile_count, one_tile, 0)

    @pl.when(pl.program_id(0) == pl.num_programs(0) - 1)
    def wait_copies():
        for copy in copies:
            copy.wait()


def tree_kernel(moment_ref, t1_ref, t2_ref, t3_ref, t4_ref, *out_refs):
    tile_count = moment_ref.shape[0]
    blocks = [moment_ref[tile] for tile in range(tile_count)]
    for block_bit, lane_bit in ((0, 2), (1, 1), (2, 0)):
        blocks = swap_bits(blocks, block_bit, lane_bit)
    blocks = run_stage(blocks, (0, 1, 2), t1_ref[...])
    for block_bit, lane_bit in ((2, 6), (1, 5), (0, 4)):
        blocks = swap_bits(blocks, block_bit, lane_bit)
    blocks = run_stage(blocks, (0, 1, 2), t2_ref[...])
    for block_bit, lane_bit in ((2, 3), (1, 2), (0, 1)):
        blocks = swap_bits(blocks, block_bit, lane_bit)
    blocks = run_stage(blocks, (0, 1, 2), t3_ref[...])
    blocks = swap_bits(blocks, 2, 0)
    blocks = run_stage(blocks, (2, 3), t4_ref[...])
    for block_bit, lane_bit in ((3, 3), (2, 4), (0, 5), (1, 6)):
        blocks = swap_bits(blocks, block_bit, lane_bit)
    for number in range(tile_count):
        place = sum((number >> bit & 1) << to for bit, to in ((1, 3), (0, 2), (2, 1), (3, 0)))
        part, column = divmod(place, tile_count // len(out_refs))
        out_refs[part][:, column * LANES : (column + 1) * LANES] = blocks[number]


def source_tables():
    first = stage_matrix(0, [2, 1, 0])
    first = np.einsum("abcd,de->abce", first, leaf_matrix())
    second = stage_matrix(3, [2, 1, 0])
    third = stage_matrix(6, [2, 1, 0])
    fourth = stage_matrix(9, [0, 1])
    return [
        jnp.asarray(split_table(table.reshape(len(table) * ROWS, -1)))
        for table in (first, second, third, fourth)
    ]


def join_kernel(own_ref, partner_ref, table_ref, out_ref, *, bit_no):
    side = lax.axis_index("leaf") >> bit_no & 1
    value = jnp.concatenate([own_ref[...], partner_ref[...]], axis=0)
    out_ref[...] = times_table(table_ref[side], value)


def join_table(tree_level, last):
    blocks = level_blocks(tree_level)
    sides = []
    for side in range(2):
        table = np.concatenate(
            [as_real(blocks[side][side]), as_real(blocks[side][1 - side])], axis=1
        )
        sides.append(split_table(field_rows() @ table if last else table))
    return jnp.asarray(np.stack(sides))


def box_rows(first):
    return pl.ds(first, 8, stride=16)


def complex_product(left, right):
    return left[0] * right[0] - left[1] * right[1], left[0] * right[1] + left[1] * right[0]


def square_of(value):
    double = 2.0 * value[1]
    return 1.0 - double * value[1], double * value[0]


def target_phases(offsets, group_cells, pair_count):
    rates = (group_cells - 1 - 2 * node_offsets(group_cells)[:HALF]) / 2.0**33
    found = [unit_circle(offsets * float(rate)) for rate in rates]
    middle = unit_circle(offsets * float((group_cells - 1) / 2.0**33))
    step = unit_circle(offsets * float(group_cells / 2.0**32))
    twice = square_of(step)
    found += [step, middle]
    for _ in range(1, pair_count):
        found.append(complex_product(found[-1], twice))
    return found


def phase_kernel(tgt_ref, after_ref, out_ref, *, first_tile, leaf_count, group_cells, pair_count):
    box_ticks = TOP_TICKS // (group_cells // BOX_CELLS)
    leaf_no = lax.axis_index("leaf")
    leaf_bits = leaf_count.bit_length() - 1
    low_box = sum((leaf_no >> bit & 1) << (leaf_bits - 1 - bit) for bit in range(leaf_bits))
    base = low_box * box_ticks + box_ticks // 2

    def one_tile(tile, carry):
        ticks = [tgt_ref[box_rows((tile + first_tile) * LANES + group), :] for group in range(16)]
        ticks = jnp.concatenate(ticks, axis=0)
        lane = lax.broadcasted_iota(jnp.int32, ticks.shape, 0)
        box = (lane & 7) * 16 + (lane >> 3) + (tile + first_tile) * LANES
        center = box * (leaf_count * box_ticks) + base
        offsets = (ticks - center).astype(jnp.float32).T
        for number, (cosine, sine) in enumerate(target_phases(offsets, group_cells, pair_count)):
            out_ref[tile, 2 * number] = cosine
            out_ref[tile, 2 * number + 1] = sine
        return carry

    lax.fori_loop(0, out_ref.shape[0], one_tile, 0)


def block_sums(phase_ref, roots, tile, first):
    totals = [None, None]
    for node in range(HALF):
        for wave in range(2):
            phase = phase_ref[tile, 2 * node + wave]
            for side in range(2):
                row = first + (2 * side + wave) * HALF + node
                term = phase * roots[pl.ds(row, 1), :]
                totals[side] = term if totals[side] is None else totals[side] + term
    return totals


def pair_field(phase_ref, root_refs, roots, sums, tile, column, pair, add_ref=None):
    low = lax.axis_index("blk") & 1
    for number, root_ref in enumerate(root_refs):
        rows = pl.ds((low ^ number) * ROWS, ROWS)
        roots[rows, :] = root_ref[:, pl.ds(pl.multiple_of(column, LANES), LANES)]
    for side, total in enumerate(block_sums(phase_ref, roots, tile, ROWS)):
        sums[side] = total
    totals = block_sums(phase_ref, roots, tile, 0)
    step = phase_ref[tile, 2 * HALF], phase_ref[tile, 2 * HALF + 1]
    real, imag = complex_product(step, (sums[0], sums[1]))
    plane = 2 * HALF + 2 + 2 * pair
    start = phase_ref[tile, plane], phase_ref[tile, plane + 1]
    values = complex_product(start, (real + totals[0], imag + totals[1]))
    for side, value in enumerate(values):
        sums[side] = value if add_ref is None else value + add_ref[side]


def near_kernel(phase_ref, *refs, first_column):
    root_refs, (out_ref, roots) = refs[:2], refs[2:]
    pair = lax.axis_index("blk") >> 1

    def one_tile(tile, carry):
        column = (tile + first_column) * LANES
        pair_field(phase_ref, root_refs, roots, out_ref.at[tile], tile, column, pair)
        return carry

    lax.fori_loop(0, out_ref.shape[0], one_tile, 0)


def far_kernel(*refs, masks):
    count = PHASE_PARTS
    phase_refs, near_refs, root_refs = refs[:count], refs[count : 2 * count], refs[2 * count : -5]
    out_ref, roots, sums, rows_ref, semaphores = refs[-5:]
    tiles = near_refs[0].shape[0]
    chunk_parts = count // CHUNKS

    def out_copy(number):
        rows = pl.ds(pl.multiple_of(number * 2 * LANES, 2 * LANES), 2 * LANES)
        return pltpu.make_async_copy(
            rows_ref.at[number], out_ref.at[rows, :], semaphores.at[number]
        )

    def make(number, tile, part):
        chunk, chunk_part = divmod(part, chunk_parts)
        column = (chunk_part * tiles + tile) * LANES
        found = root_refs[chunk * len(masks) : (chunk + 1) * len(masks)]
        add_ref = near_refs[part].at[tile]
        for first in range(0, len(masks), 2):
            pair = (lax.axis_index("blk") ^ masks[first]) >> 1
            out = sums.at[number & 1]
            pair_roots = found[first : first + 2]
            pair_field(phase_refs[part], pair_roots, roots, out, tile, column, pair, add_ref)
            add_ref = out

    def put(number):
        for side in range(2):
            values = sums[number & 1, side].T
            for group in range(16):
                rows = pl.ds(2 * group + side, 8, stride=32)
                rows_ref[number, rows, :] = values[8 * group : 8 * group + 8]

    make(0, 0, 0)
    for part in range(count):

        def one_tile(tile, carry, part=part):
            number = part * tiles + tile
            put(number - 1)
            make(number, tile, part)
            out_copy(number - 1).start()
            return carry

        lax.fori_loop(1 if part == 0 else 0, tiles, one_tile, 0)
    last = count * tiles - 1
    put(last)
    out_copy(last).start()
    for number in range(last + 1):
        out_copy(number).wait()


small_vmem = pltpu.CompilerParams(vmem_limit_bytes=6 * 2**20)


def in_vmem(value):
    return pltpu.with_memory_space_constraint(value, pltpu.VMEM)


def in_hbm(value):
    return pltpu.with_memory_space_constraint(value, pltpu.HBM)


def whole_vmem(count):
    return [pl.BlockSpec(memory_space=pltpu.VMEM)] * count


def partner_2(block, axis, apart):
    count = lax.axis_size(axis)
    route = []
    for low in range(count):
        high = low | 1 << apart
        if high != low and high < count:
            route += [(low, high), (high, low)]
    return lax.ppermute(block, axis, route)


def local(src_pos, strengths, tgt_pos):
    leaf_count = lax.axis_size("leaf")
    leaf_bits = leaf_count.bit_length() - 1
    box_count = src_pos.shape[1] // PER_BOX
    local_depth = box_count.bit_length() - 1
    assert box_count == 16 * LANES
    group_cells = box_count * leaf_count * BOX_CELLS
    box_ticks = TOP_TICKS // (box_count * leaf_count)
    offsets = node_offsets(group_cells)
    assert (offsets + offsets[::-1] == group_cells - 1).all()
    assert box_ticks // 2 * group_cells % 2**32 == 0

    tile_count = box_count // LANES
    chunk_tiles = tile_count // CHUNKS
    phase_tiles = tile_count // PHASE_PARTS

    leaf_rows = box_count // LEAF_STEPS
    tables = source_tables() + [
        join_table(local_depth + bit_no, bit_no == leaf_bits - 1) for bit_no in range(leaf_bits)
    ]
    copied = [*tables, tgt_pos.reshape(box_count, TGT_BOX)]
    moments, *copied = pl.pallas_call(
        leaf_kernel,
        grid=(LEAF_STEPS,),
        out_shape=[pltpu.VMEM((tile_count, ROWS, LANES), jnp.float32)]
        + [pltpu.VMEM(value.shape, value.dtype) for value in copied],
        in_specs=[
            pl.BlockSpec((leaf_rows, PER_BOX), lambda i: (i, 0)),
            pl.BlockSpec((2, leaf_rows, PER_BOX), lambda i: (0, i, 0)),
        ]
        + [pl.BlockSpec(memory_space=pl.ANY)] * len(copied),
        out_specs=whole_vmem(1 + len(copied)),
        scratch_shapes=[pltpu.SemaphoreType.DMA((len(copied),))],
        compiler_params=small_vmem,
        name="leaves",
    )(
        in_hbm(src_pos.reshape(box_count, PER_BOX)),
        in_hbm(strengths.reshape(2, box_count, PER_BOX)),
        *[in_hbm(value) for value in copied],
    )
    *tables, ticks = copied
    parts = pl.pallas_call(
        tree_kernel,
        out_shape=[pltpu.VMEM((ROWS, box_count // CHUNKS), jnp.float32)] * CHUNKS,
        in_specs=whole_vmem(5),
        out_specs=whole_vmem(CHUNKS),
        compiler_params=small_vmem,
        name="tree",
    )(in_vmem(moments), *[in_vmem(table) for table in tables[:-leaf_bits]])

    blk_count = lax.axis_size("blk")
    blk_bits = blk_count.bit_length() - 1
    plane_count = 2 * HALF + 2 + blk_count

    def make_phases(number, after):
        return pl.pallas_call(
            functools.partial(
                phase_kernel,
                first_tile=number * phase_tiles,
                leaf_count=leaf_count,
                group_cells=group_cells,
                pair_count=blk_count // 2,
            ),
            out_shape=pltpu.VMEM((phase_tiles, plane_count, TGT_BOX, LANES), jnp.float32),
            in_specs=whole_vmem(1) + [pl.BlockSpec(memory_space=pl.ANY)],
            out_specs=pl.BlockSpec(memory_space=pltpu.VMEM),
            compiler_params=small_vmem,
            name="phases",
        )(in_vmem(ticks), after)

    phases = []
    for bit_no in range(leaf_bits):
        table = in_vmem(tables[bit_no - leaf_bits])
        partners = [partner_2(part, "leaf", bit_no) for part in parts]
        for _ in range(PHASE_PLAN[bit_no] if bit_no < len(PHASE_PLAN) else 0):
            phases.append(make_phases(len(phases), parts[0]))
            partners[0], phases[-1] = lax.optimization_barrier((partners[0], phases[-1]))
        parts = [
            pl.pallas_call(
                functools.partial(join_kernel, bit_no=bit_no),
                out_shape=pltpu.VMEM(part.shape, jnp.float32),
                in_specs=whole_vmem(3),
                out_specs=pl.BlockSpec(memory_space=pltpu.VMEM),
                compiler_params=small_vmem,
                name="join",
            )(in_vmem(part), in_vmem(partner), table)
            for part, partner in zip(parts, partners)
        ]
    while len(phases) < PHASE_PARTS:
        phases.append(make_phases(len(phases), parts[0]))

    founds = []
    for part in parts:
        found = {0: part, 1: partner_2(part, "blk", 0)}
        for bit_no in range(1, blk_bits):
            found[1 << bit_no] = partner_2(part, "blk", bit_no)
        founds.append(found)
    parts_per_chunk = chunk_tiles // phase_tiles
    near = []
    for number, found in enumerate(founds):
        roots = lax.optimization_barrier((found[0], found[1], parts[-1]))[:2]
        for sub in range(parts_per_chunk):
            near.append(
                pl.pallas_call(
                    functools.partial(near_kernel, first_column=sub * phase_tiles),
                    out_shape=pltpu.VMEM((phase_tiles, 2, TGT_BOX, LANES), jnp.float32),
                    in_specs=whole_vmem(3),
                    out_specs=pl.BlockSpec(memory_space=pltpu.VMEM),
                    scratch_shapes=[pltpu.VMEM((2 * ROWS, LANES), jnp.float32)],
                    compiler_params=small_vmem,
                    name="near",
                )(in_vmem(phases[number * parts_per_chunk + sub]), *[in_vmem(r) for r in roots])
            )
        found[2], near[-1] = lax.optimization_barrier((found[2], near[-1]))
    masks = list(range(2, blk_count))
    for found in founds:
        for mask in masks:
            if mask not in found:
                low_bit = mask & -mask
                found[mask] = partner_2(found[mask ^ low_bit], "blk", low_bit.bit_length() - 1)
    operands = [*phases, *near, *[found[mask] for found in founds for mask in masks]]
    field = pl.pallas_call(
        functools.partial(far_kernel, masks=masks),
        out_shape=jax.ShapeDtypeStruct((2 * box_count, TGT_BOX), jnp.float32),
        in_specs=whole_vmem(len(operands)),
        out_specs=pl.BlockSpec(memory_space=pl.ANY),
        scratch_shapes=[
            pltpu.VMEM((2 * ROWS, LANES), jnp.float32),
            pltpu.VMEM((2, 2, TGT_BOX, LANES), jnp.float32),
            pltpu.VMEM((tile_count, 2 * LANES, TGT_BOX), jnp.float32),
            pltpu.SemaphoreType.DMA((tile_count,)),
        ],
        compiler_params=small_vmem,
        name="far",
    )(*[in_vmem(value) for value in operands])
    field = field.reshape(box_count, 2, TGT_BOX)
    return jnp.transpose(field, (1, 0, 2)).reshape(2, box_count * TGT_BOX)


def solution(mesh):
    return jax.shard_map(
        local,
        mesh=mesh,
        in_specs=(P("blk", "leaf"), P(None, "blk", "leaf"), P(("leaf", "blk"))),
        out_specs=P(None, ("leaf", "blk")),
        check_vma=False,
    )
```

```python
import functools

import jax
import jax.numpy as jnp
import numpy as np
from jax import lax
from jax.experimental import pallas as pl
from jax.experimental.pallas import tpu as pltpu
from jax.sharding import PartitionSpec as P


R = 16
PER_BOX = 128
TGT_BOX = 128
BOX_CELLS = 128
TOP_TICKS = 201326592
LANES = 128
ROWS = 2 * R
HALF = R // 2
CHUNKS = 2
PHASE_SHARES = ((6, 0), (2, 0), (4, 1), (4, 1))
PHASE_PLAN = {"bit_0": (0,), "bit_1": (1,), "last": (2, 3)}
LEAF_STEPS = 4

SIN_COEFS = (4.44288292, -7.30824569, 3.60635422, -0.84611165, 0.10982452)
COS_COEFS = (1.4142135, -6.97885095, 5.73946038, -1.88355791, 0.31068803)


def node_offsets(box_cells):
    node_index = np.arange(R)
    unit_nodes = (1.0 - np.cos(np.pi * (node_index + 0.5) / R)) / 2.0
    return np.floor(box_cells * unit_nodes).astype(np.int64)


def lagrange_values(node_pos, points):
    basis_rows = []
    for row_node in range(node_pos.shape[0]):
        column = np.ones(points.shape[0])
        for other_node in range(node_pos.shape[0]):
            if other_node != row_node:
                column = (
                    column
                    * (points - node_pos[other_node])
                    / (node_pos[row_node] - node_pos[other_node])
                )
        basis_rows.append(column)
    return np.stack(basis_rows)


def turn_exp(ticks, cells):
    product = (ticks * cells) % 2**32
    return np.exp(2j * np.pi * (product / 2.0**32))


def as_real(matrix):
    return np.block([[matrix.real, -matrix.imag], [matrix.imag, matrix.real]])


def level_blocks(tree_level):
    child_cells = BOX_CELLS * 2**tree_level
    box_ticks = TOP_TICKS // 2**tree_level
    assert box_ticks // 2 * child_cells % 2**32 == 0
    child_nodes = node_offsets(child_cells)
    parent_nodes = node_offsets(2 * child_cells)
    inner_cells = np.concatenate([child_nodes, child_nodes + child_cells])
    blend = lagrange_values(
        parent_nodes / (2.0 * child_cells), inner_cells / (2.0 * child_cells)
    ).reshape(R, 2, R)
    blend = blend.astype(np.float32).astype(np.float64)
    center = box_ticks // 4
    return [
        [
            blend[:, child]
            * turn_exp((2 * half - 1) * (box_ticks // 4), child_nodes)[None, :]
            * turn_exp(center, child * child_cells)
            for child in range(2)
        ]
        for half in range(2)
    ]


def stage_matrix(first_level, order):
    count = len(order)
    size = 2**count
    levels = [level_blocks(first_level + step) for step in range(count)]
    place = [order.index(step) for step in range(count)]
    full = np.zeros((size, ROWS, size, ROWS))
    for out_block in range(size):
        for in_block in range(size):
            matrix = np.eye(R)
            for step in range(count):
                bits = (out_block >> place[step] & 1, in_block >> place[step] & 1)
                matrix = levels[step][bits[0]][bits[1]] @ matrix
            full[out_block, :, in_block, :] = as_real(matrix)
    return full


def product_basis():
    table = np.zeros((R, R))
    for high in range(4):
        for low in range(4):
            for degree in (4 * high + low, abs(4 * high - low)):
                table[4 * high + low, degree] += 0.5
    return table


def leaf_matrix():
    leaf_nodes = node_offsets(BOX_CELLS)
    node_angles = np.pi * (np.arange(R) + 0.5) / R
    at_exact = lagrange_values(2.0 * leaf_nodes / BOX_CELLS - 1.0, np.cos(node_angles))
    cheb_at = np.stack([np.cos(degree * node_angles) for degree in range(R)])
    norm_weights = np.where(np.arange(R) == 0, 1.0, 2.0) / R
    coefficients = norm_weights[:, None] * (cheb_at @ at_exact.T)
    coefficients = coefficients.astype(np.float32).astype(np.float64)
    return as_real(coefficients.T @ np.linalg.inv(product_basis()))


def field_rows():
    table = np.zeros((4, HALF, 2, R))
    for node in range(HALF):
        mirror = R - 1 - node
        table[0, node, 0, [node, mirror]] = 1.0
        table[1, node, 1, [node, mirror]] = [1.0, -1.0]
        table[2, node, 1, [node, mirror]] = 1.0
        table[3, node, 0, [node, mirror]] = [-1.0, 1.0]
    return table.reshape(ROWS, ROWS)


def split_table(matrix):
    high = matrix.astype(np.float32).astype(jnp.bfloat16)
    low = (matrix - high.astype(np.float64)).astype(np.float32).astype(jnp.bfloat16)
    return np.concatenate([high, high, low], axis=-1)


def split_value(value):
    high = value.astype(jnp.bfloat16)
    low = (value - high.astype(jnp.float32)).astype(jnp.bfloat16)
    return jnp.concatenate([high, low, high], axis=0)


def times_table(table, value):
    return jnp.dot(table, split_value(value), preferred_element_type=jnp.float32)


def polynomial(coefs, value):
    total = jnp.full_like(value, coefs[-1])
    for coef in coefs[-2::-1]:
        total = total * value + coef
    return total


def unit_circle(turns):
    rest = turns - jnp.round(turns)
    square = rest * rest
    sine = rest * polynomial(SIN_COEFS, square)
    cosine = polynomial(COS_COEFS, square)
    return 1.0 - sine * sine, sine * cosine


def reverse_bits(value, count):
    return sum((value >> bit & 1) << (count - 1 - bit) for bit in range(count))


def swap_bits(blocks, block_bit, lane_bit):
    step = 1 << lane_bit
    shape = blocks[0].shape
    upper = (lax.broadcasted_iota(jnp.int32, shape, 1) >> lane_bit & 1) == 1
    swapped = list(blocks)
    for number in range(len(blocks)):
        if not number >> block_bit & 1:
            other = number | 1 << block_bit
            low, high = blocks[number], blocks[other]
            swapped[number] = jnp.where(upper, pltpu.roll(high, step, 1), low)
            swapped[other] = jnp.where(upper, high, pltpu.roll(low, LANES - step, 1))
    return swapped


def run_stage(blocks, row_bits, table):
    count = len(blocks)
    side_bits = [bit for bit in range(count.bit_length() - 1) if bit not in row_bits]

    def number(row, side):
        return sum((row >> k & 1) << bit for k, bit in enumerate(row_bits)) + sum(
            (side >> k & 1) << bit for k, bit in enumerate(side_bits)
        )

    sides = range(2 ** len(side_bits))
    rows = range(2 ** len(row_bits))
    value = jnp.concatenate(
        [
            jnp.concatenate([blocks[number(row, side)] for row in rows], axis=0)
            for side in sides
        ],
        axis=1,
    )
    product = times_table(table, value)
    result = list(blocks)
    for side in sides:
        for row in rows:
            result[number(row, side)] = product[
                row * ROWS : (row + 1) * ROWS, side * LANES : (side + 1) * LANES
            ]
    return result


def cell_table():
    turned = turn_exp(TOP_TICKS // 2, np.arange(BOX_CELLS))
    return jnp.asarray(np.repeat([turned.real, turned.imag], 8, axis=0), jnp.float32)


def pick_lanes(table, lanes):
    numbers = lax.GatherDimensionNumbers(
        offset_dims=(),
        collapsed_slice_dims=(1,),
        start_index_map=(1,),
        operand_batching_dims=(0,),
        start_indices_batching_dims=(0,),
    )
    return lax.gather(
        table, lanes[..., None], numbers, (1, 1), mode=lax.GatherScatterMode.PROMISE_IN_BOUNDS
    )


def leaf_kernel(pos_ref, strength_ref, table_ref, *refs):
    count = (len(refs) - 2) // 2
    out_ref, semaphores = refs[count], refs[-1]
    copies = [
        pltpu.make_async_copy(source, target, semaphores.at[number])
        for number, (source, target) in enumerate(zip(refs[:count], refs[count + 1 : -1]))
    ]

    @pl.when(pl.program_id(0) == 0)
    def start_copies():
        for copy in copies:
            copy.start()

    tile_count = pos_ref.shape[0] // LANES
    first = pl.program_id(0) * tile_count

    def one_tile(tile, carry):
        parts = [[], [], []]
        for group in range(16):
            start = tile * LANES + 8 * reverse_bits(group, 4)
            rows = pl.ds(pl.multiple_of(start, 8), 8)
            parts[0].append(pos_ref[rows, :] & (BOX_CELLS - 1))
            parts[1].append(strength_ref[0, rows, :])
            parts[2].append(strength_ref[1, rows, :])
        cells, real, imag = (jnp.concatenate(part, axis=0).T for part in parts)
        sums = [None] * ROWS
        for group in range(16):
            rows = slice(8 * group, 8 * group + 8)
            turn = [pick_lanes(table_ref[8 * row : 8 * row + 8, :], cells[rows]) for row in range(2)]
            turned = complex_product(turn, (real[rows], imag[rows]))
            v = cells[rows].astype(jnp.float32) * (2.0 / BOX_CELLS) - 1.0
            t2 = 2.0 * (v * v) - 1.0
            t3 = v * (2.0 * t2 - 1.0)
            t4 = 2.0 * (t2 * t2) - 1.0
            t8 = 2.0 * (t4 * t4) - 1.0
            t12 = t4 * (2.0 * t8 - 1.0)
            for side, value in enumerate(turned):
                for high, outer in enumerate((None, t4, t8, t12)):
                    base = value if outer is None else value * outer
                    for low, inner in enumerate((None, v, t2, t3)):
                        term = base if inner is None else base * inner
                        row = side * R + 4 * high + low
                        sums[row] = term if sums[row] is None else sums[row] + term
        for row in range(ROWS):
            out_ref[first + tile, pl.ds(row, 1), :] = jnp.sum(sums[row], axis=0, keepdims=True)
        return carry

    lax.fori_loop(0, tile_count, one_tile, 0, unroll=4)

    @pl.when(pl.program_id(0) == pl.num_programs(0) - 1)
    def wait_copies():
        for copy in copies:
            copy.wait()


def tree_kernel(moment_ref, t1_ref, t2_ref, t3_ref, t4_ref, *out_refs):
    tile_count = moment_ref.shape[0]
    blocks = [moment_ref[tile] for tile in range(tile_count)]
    for block_bit, lane_bit in ((0, 2), (1, 1), (2, 0)):
        blocks = swap_bits(blocks, block_bit, lane_bit)
    blocks = run_stage(blocks, (0, 1, 2), t1_ref[...])
    for block_bit, lane_bit in ((2, 6), (1, 5), (0, 4)):
        blocks = swap_bits(blocks, block_bit, lane_bit)
    blocks = run_stage(blocks, (0, 1, 2), t2_ref[...])
    for block_bit, lane_bit in ((2, 3), (1, 2), (0, 1)):
        blocks = swap_bits(blocks, block_bit, lane_bit)
    blocks = run_stage(blocks, (0, 1, 2), t3_ref[...])
    blocks = swap_bits(blocks, 2, 0)
    blocks = run_stage(blocks, (2, 3), t4_ref[...])
    for block_bit, lane_bit in ((3, 3), (2, 4), (0, 5), (1, 6)):
        blocks = swap_bits(blocks, block_bit, lane_bit)
    for number in range(tile_count):
        place = sum((number >> bit & 1) << to for bit, to in ((1, 3), (0, 2), (2, 1), (3, 0)))
        part, column = divmod(place, tile_count // len(out_refs))
        out_refs[part][:, column * LANES : (column + 1) * LANES] = blocks[number]


def source_tables():
    first = stage_matrix(0, [2, 1, 0])
    first = np.einsum("abcd,de->abce", first, leaf_matrix())
    second = stage_matrix(3, [2, 1, 0])
    third = stage_matrix(6, [2, 1, 0])
    fourth = stage_matrix(9, [0, 1])
    return [
        jnp.asarray(split_table(table.reshape(len(table) * ROWS, -1)))
        for table in (first, second, third, fourth)
    ]


def join_kernel(own_ref, partner_ref, table_ref, out_ref, *, bit_no):
    side = lax.axis_index("leaf") >> bit_no & 1
    value = jnp.concatenate([own_ref[...], partner_ref[...]], axis=0)
    out_ref[...] = times_table(table_ref[side], value)


def join_table(tree_level, last):
    blocks = level_blocks(tree_level)
    sides = []
    for side in range(2):
        table = np.concatenate(
            [as_real(blocks[side][side]), as_real(blocks[side][1 - side])], axis=1
        )
        sides.append(split_table(field_rows() @ table if last else table))
    return jnp.asarray(np.stack(sides))


def box_rows(first):
    return pl.ds(first, 8, stride=16)


def complex_product(left, right):
    return left[0] * right[0] - left[1] * right[1], left[0] * right[1] + left[1] * right[0]


def square_of(value):
    double = 2.0 * value[1]
    return 1.0 - double * value[1], double * value[0]


def target_phases(offsets, group_cells, pair_count):
    rates = (group_cells - 1 - 2 * node_offsets(group_cells)[:HALF]) / 2.0**33
    found = [unit_circle(offsets * float(rate)) for rate in rates]
    middle = unit_circle(offsets * float((group_cells - 1) / 2.0**33))
    step = unit_circle(offsets * float(group_cells / 2.0**32))
    twice = square_of(step)
    found += [step, middle]
    for _ in range(1, pair_count):
        found.append(complex_product(found[-1], twice))
    return found


def phase_kernel(tgt_ref, after_ref, out_ref, *, first_tile, leaf_count, group_cells, pair_count):
    box_ticks = TOP_TICKS // (group_cells // BOX_CELLS)
    leaf_no = lax.axis_index("leaf")
    leaf_bits = leaf_count.bit_length() - 1
    low_box = sum((leaf_no >> bit & 1) << (leaf_bits - 1 - bit) for bit in range(leaf_bits))
    base = low_box * box_ticks + box_ticks // 2

    def one_tile(tile, carry):
        ticks = [tgt_ref[box_rows((tile + first_tile) * LANES + group), :] for group in range(16)]
        ticks = jnp.concatenate(ticks, axis=0)
        lane = lax.broadcasted_iota(jnp.int32, ticks.shape, 0)
        box = (lane & 7) * 16 + (lane >> 3) + (tile + first_tile) * LANES
        center = box * (leaf_count * box_ticks) + base
        offsets = (ticks - center).astype(jnp.float32).T
        for number, (cosine, sine) in enumerate(target_phases(offsets, group_cells, pair_count)):
            out_ref[tile, 2 * number] = cosine
            out_ref[tile, 2 * number + 1] = sine
        return carry

    lax.fori_loop(0, out_ref.shape[0], one_tile, 0, unroll=2)


def block_sums(phase_ref, roots, tile, first):
    totals = [None, None]
    for node in range(HALF):
        for wave in range(2):
            phase = phase_ref[tile, 2 * node + wave]
            for side in range(2):
                row = first + (2 * side + wave) * HALF + node
                term = phase * roots[pl.ds(row, 1), :]
                totals[side] = term if totals[side] is None else totals[side] + term
    return totals


def pair_field(phase_ref, root_refs, roots, sums, tile, column, pair, add_ref=None):
    low = lax.axis_index("blk") & 1
    for number, root_ref in enumerate(root_refs):
        rows = pl.ds((low ^ number) * ROWS, ROWS)
        roots[rows, :] = root_ref[:, pl.ds(pl.multiple_of(column, LANES), LANES)]
    for side, total in enumerate(block_sums(phase_ref, roots, tile, ROWS)):
        sums[side] = total
    totals = block_sums(phase_ref, roots, tile, 0)
    step = phase_ref[tile, 2 * HALF], phase_ref[tile, 2 * HALF + 1]
    real, imag = complex_product(step, (sums[0], sums[1]))
    plane = 2 * HALF + 2 + 2 * pair
    start = phase_ref[tile, plane], phase_ref[tile, plane + 1]
    values = complex_product(start, (real + totals[0], imag + totals[1]))
    for side, value in enumerate(values):
        sums[side] = value if add_ref is None else value + add_ref[side]


def near_kernel(phase_ref, *refs, first_column):
    root_refs, (out_ref, roots) = refs[:2], refs[2:]
    pair = lax.axis_index("blk") >> 1

    def one_tile(tile, carry):
        column = (tile + first_column) * LANES
        pair_field(phase_ref, root_refs, roots, out_ref.at[tile], tile, column, pair)
        return carry

    lax.fori_loop(0, out_ref.shape[0], one_tile, 0)


def share_places(tile_counts):
    firsts = [sum(tile_counts[:part]) for part in range(len(tile_counts))]
    starts = {}
    for (_, chunk), first in zip(PHASE_SHARES, firsts):
        starts.setdefault(chunk, first)
    return firsts, [first - starts[chunk] for (_, chunk), first in zip(PHASE_SHARES, firsts)]


def far_kernel(*refs, masks):
    count = len(PHASE_SHARES)
    phase_refs, near_refs, root_refs = refs[:count], refs[count : 2 * count], refs[2 * count : -5]
    out_ref, roots, sums, rows_ref, semaphores = refs[-5:]
    firsts, places = share_places([near_ref.shape[0] for near_ref in near_refs])

    def out_copy(number):
        rows = pl.ds(pl.multiple_of(number * 2 * LANES, 2 * LANES), 2 * LANES)
        return pltpu.make_async_copy(
            rows_ref.at[number], out_ref.at[rows, :], semaphores.at[number]
        )

    def make(number, tile, part):
        chunk = PHASE_SHARES[part][1]
        column = (places[part] + tile) * LANES
        found = root_refs[chunk * len(masks) : (chunk + 1) * len(masks)]
        add_ref = near_refs[part].at[tile]
        for first in range(0, len(masks), 2):
            pair = (lax.axis_index("blk") ^ masks[first]) >> 1
            out = sums.at[number & 1]
            pair_roots = found[first : first + 2]
            pair_field(phase_refs[part], pair_roots, roots, out, tile, column, pair, add_ref)
            add_ref = out

    def put(number):
        for side in range(2):
            values = sums[number & 1, side].T
            for group in range(16):
                rows = pl.ds(2 * group + side, 8, stride=32)
                rows_ref[number, rows, :] = values[8 * group : 8 * group + 8]

    make(0, 0, 0)
    for part in range(count):

        def one_tile(tile, carry, part=part):
            number = firsts[part] + tile
            put(number - 1)
            make(number, tile, part)
            out_copy(number - 1).start()
            return carry

        lax.fori_loop(1 if part == 0 else 0, near_refs[part].shape[0], one_tile, 0)
    last = rows_ref.shape[0] - 1
    put(last)
    out_copy(last).start()
    for number in range(last + 1):
        out_copy(number).wait()


small_vmem = pltpu.CompilerParams(vmem_limit_bytes=6 * 2**20)


def in_vmem(value):
    return pltpu.with_memory_space_constraint(value, pltpu.VMEM)


def in_hbm(value):
    return pltpu.with_memory_space_constraint(value, pltpu.HBM)


def whole_vmem(count):
    return [pl.BlockSpec(memory_space=pltpu.VMEM)] * count


def partner_2(block, axis, apart):
    count = lax.axis_size(axis)
    route = []
    for low in range(count):
        high = low | 1 << apart
        if high != low and high < count:
            route += [(low, high), (high, low)]
    return lax.ppermute(block, axis, route)


def local(src_pos, strengths, tgt_pos):
    leaf_count = lax.axis_size("leaf")
    leaf_bits = leaf_count.bit_length() - 1
    box_count = src_pos.shape[1] // PER_BOX
    local_depth = box_count.bit_length() - 1
    assert box_count == 16 * LANES
    group_cells = box_count * leaf_count * BOX_CELLS
    box_ticks = TOP_TICKS // (box_count * leaf_count)
    offsets = node_offsets(group_cells)
    assert (offsets + offsets[::-1] == group_cells - 1).all()
    assert box_ticks // 2 * group_cells % 2**32 == 0

    tile_count = box_count // LANES
    part_tiles = [tile_count * share // 16 for share, _ in PHASE_SHARES]
    firsts, places = share_places(part_tiles)

    leaf_rows = box_count // LEAF_STEPS
    tables = source_tables() + [
        join_table(local_depth + bit_no, bit_no == leaf_bits - 1) for bit_no in range(leaf_bits)
    ]
    copied = [*tables, tgt_pos.reshape(box_count, TGT_BOX)]
    moments, *copied = pl.pallas_call(
        leaf_kernel,
        grid=(LEAF_STEPS,),
        out_shape=[pltpu.VMEM((tile_count, ROWS, LANES), jnp.float32)]
        + [pltpu.VMEM(value.shape, value.dtype) for value in copied],
        in_specs=[
            pl.BlockSpec((leaf_rows, PER_BOX), lambda i: (i, 0)),
            pl.BlockSpec((2, leaf_rows, PER_BOX), lambda i: (0, i, 0)),
            pl.BlockSpec((16, BOX_CELLS), lambda i: (0, 0)),
        ]
        + [pl.BlockSpec(memory_space=pl.ANY)] * len(copied),
        out_specs=whole_vmem(1 + len(copied)),
        scratch_shapes=[pltpu.SemaphoreType.DMA((len(copied),))],
        compiler_params=small_vmem,
        name="leaves",
    )(
        in_hbm(src_pos.reshape(box_count, PER_BOX)),
        in_hbm(strengths.reshape(2, box_count, PER_BOX)),
        in_hbm(cell_table()),
        *[in_hbm(value) for value in copied],
    )
    *tables, ticks = copied
    parts = pl.pallas_call(
        tree_kernel,
        out_shape=[pltpu.VMEM((ROWS, box_count // CHUNKS), jnp.float32)] * CHUNKS,
        in_specs=whole_vmem(5),
        out_specs=whole_vmem(CHUNKS),
        compiler_params=small_vmem,
        name="tree",
    )(in_vmem(moments), *[in_vmem(table) for table in tables[:-leaf_bits]])

    blk_count = lax.axis_size("blk")
    blk_bits = blk_count.bit_length() - 1
    plane_count = 2 * HALF + 2 + blk_count

    def make_phases(number, after):
        return pl.pallas_call(
            functools.partial(
                phase_kernel,
                first_tile=firsts[number],
                leaf_count=leaf_count,
                group_cells=group_cells,
                pair_count=blk_count // 2,
            ),
            out_shape=pltpu.VMEM((part_tiles[number], plane_count, TGT_BOX, LANES), jnp.float32),
            in_specs=whole_vmem(1) + [pl.BlockSpec(memory_space=pl.ANY)],
            out_specs=pl.BlockSpec(memory_space=pltpu.VMEM),
            compiler_params=small_vmem,
            name="phases",
        )(in_vmem(ticks), after)

    def join(part, partner, bit_no):
        return pl.pallas_call(
            functools.partial(join_kernel, bit_no=bit_no),
            out_shape=pltpu.VMEM(part.shape, jnp.float32),
            in_specs=whole_vmem(3),
            out_specs=pl.BlockSpec(memory_space=pltpu.VMEM),
            compiler_params=small_vmem,
            name="join",
        )(in_vmem(part), in_vmem(partner), in_vmem(tables[bit_no - leaf_bits]))

    def near_field(number, roots):
        return pl.pallas_call(
            functools.partial(near_kernel, first_column=places[number]),
            out_shape=pltpu.VMEM((part_tiles[number], 2, TGT_BOX, LANES), jnp.float32),
            in_specs=whole_vmem(3),
            out_specs=pl.BlockSpec(memory_space=pltpu.VMEM),
            scratch_shapes=[pltpu.VMEM((2 * ROWS, LANES), jnp.float32)],
            compiler_params=small_vmem,
            name="near",
        )(in_vmem(phases[number]), *[in_vmem(root) for root in roots])

    phases = []
    for bit_no in range(leaf_bits):
        stage = "last" if bit_no == leaf_bits - 1 else f"bit_{bit_no}"
        partners = []
        for part in parts:
            partners.append(partner_2(part, "leaf", bit_no))
        for number in PHASE_PLAN.get(stage, ()):
            phases.append(make_phases(number, parts[0]))
            partners[0], phases[-1] = lax.optimization_barrier((partners[0], phases[-1]))
        joined = []
        for part, partner in zip(parts, partners):
            joined.append(join(part, partner, bit_no))
        parts = joined
    masks = list(range(2, blk_count))
    founds = []
    for part in parts:
        found = {0: part, 1: partner_2(part, "blk", 0)}
        for blk_bit in range(1, blk_bits):
            found[1 << blk_bit] = partner_2(part, "blk", blk_bit)
        founds.append(found)
    near = []
    for number, (_, chunk) in enumerate(PHASE_SHARES):
        near.append(near_field(number, (founds[chunk][0], founds[chunk][1])))
    founds[0][2], *near[:3] = lax.optimization_barrier((founds[0][2], *near[:3]))
    founds[1][2], near[3] = lax.optimization_barrier((founds[1][2], near[3]))
    for found in founds:
        for mask in masks:
            if mask not in found:
                low_bit = mask & -mask
                found[mask] = partner_2(
                    found[mask ^ low_bit], "blk", low_bit.bit_length() - 1
                )
    operands = [*phases, *near, *[found[mask] for found in founds for mask in masks]]
    field = pl.pallas_call(
        functools.partial(far_kernel, masks=masks),
        out_shape=jax.ShapeDtypeStruct((2 * box_count, TGT_BOX), jnp.float32),
        in_specs=whole_vmem(len(operands)),
        out_specs=pl.BlockSpec(memory_space=pl.ANY),
        scratch_shapes=[
            pltpu.VMEM((2 * ROWS, LANES), jnp.float32),
            pltpu.VMEM((2, 2, TGT_BOX, LANES), jnp.float32),
            pltpu.VMEM((tile_count, 2 * LANES, TGT_BOX), jnp.float32),
            pltpu.SemaphoreType.DMA((tile_count,)),
        ],
        compiler_params=small_vmem,
        name="far",
    )(*[in_vmem(value) for value in operands])
    field = field.reshape(box_count, 2, TGT_BOX)
    return jnp.transpose(field, (1, 0, 2)).reshape(2, box_count * TGT_BOX)


def solution(mesh):
    return jax.shard_map(
        local,
        mesh=mesh,
        in_specs=(P("blk", "leaf"), P(None, "blk", "leaf"), P(("leaf", "blk"))),
        out_specs=P(None, ("leaf", "blk")),
        check_vma=False,
    )
```

```python
import functools

import jax
import jax.numpy as jnp
import numpy as np
from jax import lax
from jax.experimental import pallas as pl
from jax.experimental.pallas import tpu as pltpu
from jax.sharding import PartitionSpec as P


R = 16
PER_BOX = 128
TGT_BOX = 128
BOX_CELLS = 128
TOP_TICKS = 201326592
LANES = 128
ROWS = 2 * R
HALF = R // 2
CHUNKS = 2
PHASE_SHARES = ((6, 0), (2, 0), (4, 1), (2, 1), (2, 1))
PHASE_PLAN = {"bit_0": (0,), "bit_1": (1,), "last": (2, 3, 4)}
LEAF_STEPS = 4
LEAF_AHEAD = 2
ROW_CHUNK = 64

SIN_COEFS = (4.44288292, -7.30824569, 3.60635422, -0.84611165, 0.10982452)
COS_COEFS = (1.4142135, -6.97885095, 5.73946038, -1.88355791, 0.31068803)


def node_offsets(box_cells):
    node_index = np.arange(R)
    unit_nodes = (1.0 - np.cos(np.pi * (node_index + 0.5) / R)) / 2.0
    return np.floor(box_cells * unit_nodes).astype(np.int64)


def lagrange_values(node_pos, points):
    basis_rows = []
    for row_node in range(node_pos.shape[0]):
        column = np.ones(points.shape[0])
        for other_node in range(node_pos.shape[0]):
            if other_node != row_node:
                column = (
                    column
                    * (points - node_pos[other_node])
                    / (node_pos[row_node] - node_pos[other_node])
                )
        basis_rows.append(column)
    return np.stack(basis_rows)


def turn_exp(ticks, cells):
    product = (ticks * cells) % 2**32
    return np.exp(2j * np.pi * (product / 2.0**32))


def as_real(matrix):
    return np.block([[matrix.real, -matrix.imag], [matrix.imag, matrix.real]])


def level_blocks(tree_level):
    child_cells = BOX_CELLS * 2**tree_level
    box_ticks = TOP_TICKS // 2**tree_level
    assert box_ticks // 2 * child_cells % 2**32 == 0
    child_nodes = node_offsets(child_cells)
    parent_nodes = node_offsets(2 * child_cells)
    inner_cells = np.concatenate([child_nodes, child_nodes + child_cells])
    blend = lagrange_values(
        parent_nodes / (2.0 * child_cells), inner_cells / (2.0 * child_cells)
    ).reshape(R, 2, R)
    blend = blend.astype(np.float32).astype(np.float64)
    center = box_ticks // 4
    return [
        [
            blend[:, child]
            * turn_exp((2 * half - 1) * (box_ticks // 4), child_nodes)[None, :]
            * turn_exp(center, child * child_cells)
            for child in range(2)
        ]
        for half in range(2)
    ]


def stage_matrix(first_level, order):
    count = len(order)
    size = 2**count
    levels = [level_blocks(first_level + step) for step in range(count)]
    place = [order.index(step) for step in range(count)]
    full = np.zeros((size, ROWS, size, ROWS))
    for out_block in range(size):
        for in_block in range(size):
            matrix = np.eye(R)
            for step in range(count):
                bits = (out_block >> place[step] & 1, in_block >> place[step] & 1)
                matrix = levels[step][bits[0]][bits[1]] @ matrix
            full[out_block, :, in_block, :] = as_real(matrix)
    return full


def product_basis():
    table = np.zeros((R, R))
    for high in range(4):
        for low in range(4):
            for degree in (4 * high + low, abs(4 * high - low)):
                table[4 * high + low, degree] += 0.5
    return table


def leaf_matrix():
    leaf_nodes = node_offsets(BOX_CELLS)
    node_angles = np.pi * (np.arange(R) + 0.5) / R
    at_exact = lagrange_values(2.0 * leaf_nodes / BOX_CELLS - 1.0, np.cos(node_angles))
    cheb_at = np.stack([np.cos(degree * node_angles) for degree in range(R)])
    norm_weights = np.where(np.arange(R) == 0, 1.0, 2.0) / R
    coefficients = norm_weights[:, None] * (cheb_at @ at_exact.T)
    coefficients = coefficients.astype(np.float32).astype(np.float64)
    return as_real(coefficients.T @ np.linalg.inv(product_basis()))


def field_rows():
    table = np.zeros((4, HALF, 2, R))
    for node in range(HALF):
        mirror = R - 1 - node
        table[0, node, 0, [node, mirror]] = 1.0
        table[1, node, 1, [node, mirror]] = [1.0, -1.0]
        table[2, node, 1, [node, mirror]] = 1.0
        table[3, node, 0, [node, mirror]] = [-1.0, 1.0]
    return table.reshape(ROWS, ROWS)


def split_table(matrix):
    high = matrix.astype(np.float32).astype(jnp.bfloat16)
    low = (matrix - high.astype(np.float64)).astype(np.float32).astype(jnp.bfloat16)
    return np.concatenate([high, high, low], axis=-1)


def split_value(value):
    high = value.astype(jnp.bfloat16)
    low = (value - high.astype(jnp.float32)).astype(jnp.bfloat16)
    return jnp.concatenate([high, low, high], axis=0)


def times_table(table, value):
    return jnp.dot(table, split_value(value), preferred_element_type=jnp.float32)


def polynomial(coefs, value):
    total = jnp.full_like(value, coefs[-1])
    for coef in coefs[-2::-1]:
        total = total * value + coef
    return total


def unit_circle(turns):
    rest = turns - jnp.round(turns)
    square = rest * rest
    sine = rest * polynomial(SIN_COEFS, square)
    cosine = polynomial(COS_COEFS, square)
    return 1.0 - sine * sine, sine * cosine


def reverse_bits(value, count):
    return sum((value >> bit & 1) << (count - 1 - bit) for bit in range(count))


def swap_bits(blocks, block_bit, lane_bit):
    lane = lax.broadcasted_iota(jnp.int32, (8, LANES), 1)
    upper = (lax.broadcasted_iota(jnp.int32, blocks[0].shape, 1) >> lane_bit & 1) == 1
    swapped = list(blocks)
    for number in range(len(blocks)):
        if not number >> block_bit & 1:
            other = number | 1 << block_bit
            low, high = blocks[number], blocks[other]
            mixed = jnp.where(upper, low, high)
            moved = jnp.concatenate(
                [pick_lanes(mixed[row : row + 8], lane ^ 1 << lane_bit) for row in range(0, ROWS, 8)],
                axis=0,
            )
            swapped[number] = jnp.where(upper, moved, low)
            swapped[other] = jnp.where(upper, high, moved)
    return swapped


def run_stage(blocks, row_bits, table):
    count = len(blocks)
    side_bits = [bit for bit in range(count.bit_length() - 1) if bit not in row_bits]

    def number(row, side):
        return sum((row >> k & 1) << bit for k, bit in enumerate(row_bits)) + sum(
            (side >> k & 1) << bit for k, bit in enumerate(side_bits)
        )

    sides = range(2 ** len(side_bits))
    rows = range(2 ** len(row_bits))
    value = jnp.concatenate(
        [
            jnp.concatenate([blocks[number(row, side)] for row in rows], axis=0)
            for side in sides
        ],
        axis=1,
    )
    product = times_table(table, value)
    result = list(blocks)
    for side in sides:
        for row in rows:
            result[number(row, side)] = product[
                row * ROWS : (row + 1) * ROWS, side * LANES : (side + 1) * LANES
            ]
    return result


def cell_table():
    turned = turn_exp(TOP_TICKS // 2, np.arange(BOX_CELLS))
    return jnp.asarray(np.repeat([turned.real, turned.imag], 8, axis=0), jnp.float32)


def pick_lanes(table, lanes):
    numbers = lax.GatherDimensionNumbers(
        offset_dims=(),
        collapsed_slice_dims=(1,),
        start_index_map=(1,),
        operand_batching_dims=(0,),
        start_indices_batching_dims=(0,),
    )
    return lax.gather(
        table, lanes[..., None], numbers, (1, 1), mode=lax.GatherScatterMode.PROMISE_IN_BOUNDS
    )


def sublane_sums(values):
    sublane = lax.broadcasted_iota(jnp.int32, (8, LANES), 0)
    for step in (4, 2, 1):
        lower = (sublane & step) == 0
        values = [
            jnp.where(lower, first, second)
            + pltpu.roll(jnp.where(lower, second, first), step, 0)
            if step == 4
            else jnp.where(lower, first, second)
            + jnp.where(lower, pltpu.roll(first, 8 - step, 0), pltpu.roll(second, step, 0))
            for first, second in zip(values[:step], values[step:])
        ]
    return values[0]


def leaf_kernel(pos_hbm, strength_hbm, table_hbm, *refs):
    count = (len(refs) - 8) // 2
    out_ref, pos_ref, strength_ref, table_ref = refs[count], *refs[2 * count + 1 : 2 * count + 4]
    pos_done, strength_done, table_done, other_done = refs[2 * count + 4 :]
    others = [
        pltpu.make_async_copy(source, target, other_done.at[number])
        for number, (source, target) in enumerate(zip(refs[:count], refs[count + 1 :]))
    ]
    table_copy = pltpu.make_async_copy(table_hbm, table_ref, table_done)
    size = pos_ref.shape[0] // LEAF_STEPS

    def step_copies(step):
        rows = pl.ds(pl.multiple_of(step * size, LANES), size)
        yield pltpu.make_async_copy(pos_hbm.at[rows, :], pos_ref.at[rows, :], pos_done.at[step])
        yield pltpu.make_async_copy(
            strength_hbm.at[:, rows, :], strength_ref.at[:, rows, :], strength_done.at[step]
        )

    table_copy.start()
    for step in range(LEAF_AHEAD):
        for copy in step_copies(step):
            copy.start()

    def one_tile(tile):
        parts = [[], [], []]
        for group in range(16):
            start = tile * LANES + 8 * reverse_bits(group, 4)
            rows = pl.ds(pl.multiple_of(start, 8), 8)
            parts[0].append(pos_ref[rows, :] & (BOX_CELLS - 1))
            parts[1].append(strength_ref[0, rows, :])
            parts[2].append(strength_ref[1, rows, :])
        cells, real, imag = (jnp.concatenate(part, axis=0).T for part in parts)
        sums = [None] * ROWS
        for group in range(16):
            rows = slice(8 * group, 8 * group + 8)
            turn = [pick_lanes(table_ref[8 * row : 8 * row + 8, :], cells[rows]) for row in range(2)]
            turned = complex_product(turn, (real[rows], imag[rows]))
            v = cells[rows].astype(jnp.float32) * (2.0 / BOX_CELLS) - 1.0
            t2 = 2.0 * (v * v) - 1.0
            t3 = v * (2.0 * t2 - 1.0)
            t4 = 2.0 * (t2 * t2) - 1.0
            t8 = 2.0 * (t4 * t4) - 1.0
            t12 = t4 * (2.0 * t8 - 1.0)
            for side, value in enumerate(turned):
                for high, outer in enumerate((None, t4, t8, t12)):
                    base = value if outer is None else value * outer
                    for low, inner in enumerate((None, v, t2, t3)):
                        term = base if inner is None else base * inner
                        row = side * R + 4 * high + low
                        sums[row] = term if sums[row] is None else sums[row] + term
        for row in range(0, ROWS, 8):
            out_ref[tile, pl.ds(row, 8), :] = sublane_sums(sums[row : row + 8])

    def one_step(step, carry):
        for copy in step_copies(step):
            copy.wait()

        @pl.when(step < LEAF_STEPS - LEAF_AHEAD)
        def start_later():
            for copy in step_copies(step + LEAF_AHEAD):
                copy.start()

        @pl.when(step == LEAF_STEPS - LEAF_AHEAD)
        def start_others():
            for copy in others:
                copy.start()

        for tile in range(size // LANES):
            one_tile(step * (size // LANES) + tile)
        return carry

    table_copy.wait()
    lax.fori_loop(0, LEAF_STEPS, one_step, 0)
    for copy in others:
        copy.wait()


def tree_kernel(moment_ref, t1_ref, t2_ref, t3_ref, t4_ref, *out_refs):
    tile_count = moment_ref.shape[0]
    blocks = [moment_ref[tile] for tile in range(tile_count)]
    for block_bit, lane_bit in ((0, 2), (1, 1), (2, 0)):
        blocks = swap_bits(blocks, block_bit, lane_bit)
    blocks = run_stage(blocks, (0, 1, 2), t1_ref[...])
    for block_bit, lane_bit in ((2, 6), (1, 5), (0, 4)):
        blocks = swap_bits(blocks, block_bit, lane_bit)
    blocks = run_stage(blocks, (0, 1, 2), t2_ref[...])
    for block_bit, lane_bit in ((2, 3), (1, 2), (0, 1)):
        blocks = swap_bits(blocks, block_bit, lane_bit)
    blocks = run_stage(blocks, (0, 1, 2), t3_ref[...])
    blocks = swap_bits(blocks, 2, 0)
    blocks = run_stage(blocks, (2, 3), t4_ref[...])
    for block_bit, lane_bit in ((3, 3), (2, 4), (0, 5), (1, 6)):
        blocks = swap_bits(blocks, block_bit, lane_bit)
    for number in range(tile_count):
        place = sum((number >> bit & 1) << to for bit, to in ((1, 3), (0, 2), (2, 1), (3, 0)))
        part, column = divmod(place, tile_count // len(out_refs))
        out_refs[part][:, column * LANES : (column + 1) * LANES] = blocks[number]


def source_tables():
    first = stage_matrix(0, [2, 1, 0])
    first = np.einsum("abcd,de->abce", first, leaf_matrix())
    second = stage_matrix(3, [2, 1, 0])
    third = stage_matrix(6, [2, 1, 0])
    fourth = stage_matrix(9, [0, 1])
    return [
        jnp.asarray(split_table(table.reshape(len(table) * ROWS, -1)))
        for table in (first, second, third, fourth)
    ]


def join_kernel(own_ref, partner_ref, table_ref, out_ref, *, bit_no):
    side = lax.axis_index("leaf") >> bit_no & 1
    value = jnp.concatenate([own_ref[...], partner_ref[...]], axis=0)
    out_ref[...] = times_table(table_ref[side], value)


def join_table(tree_level, last):
    blocks = level_blocks(tree_level)
    sides = []
    for side in range(2):
        table = np.concatenate(
            [as_real(blocks[side][side]), as_real(blocks[side][1 - side])], axis=1
        )
        sides.append(split_table(field_rows() @ table if last else table))
    return jnp.asarray(np.stack(sides))


def box_rows(first):
    return pl.ds(first, 8, stride=16)


def complex_product(left, right):
    return left[0] * right[0] - left[1] * right[1], left[0] * right[1] + left[1] * right[0]


def square_of(value):
    double = 2.0 * value[1]
    return 1.0 - double * value[1], double * value[0]


def target_phases(offsets, group_cells, pair_count):
    rates = (group_cells - 1 - 2 * node_offsets(group_cells)[:HALF]) / 2.0**33
    found = [unit_circle(offsets * float(rate)) for rate in rates]
    middle = unit_circle(offsets * float((group_cells - 1) / 2.0**33))
    step = unit_circle(offsets * float(group_cells / 2.0**32))
    twice = square_of(step)
    found += [step, middle]
    for _ in range(1, pair_count):
        found.append(complex_product(found[-1], twice))
    return found


def phase_kernel(tgt_ref, after_ref, out_ref, *, first_tile, leaf_count, group_cells, pair_count):
    box_ticks = TOP_TICKS // (group_cells // BOX_CELLS)
    leaf_no = lax.axis_index("leaf")
    leaf_bits = leaf_count.bit_length() - 1
    low_box = sum((leaf_no >> bit & 1) << (leaf_bits - 1 - bit) for bit in range(leaf_bits))
    base = low_box * box_ticks + box_ticks // 2

    def one_tile(tile, carry):
        ticks = [tgt_ref[box_rows((tile + first_tile) * LANES + group), :] for group in range(16)]
        ticks = jnp.concatenate(ticks, axis=0)
        lane = lax.broadcasted_iota(jnp.int32, ticks.shape, 0)
        box = (lane & 7) * 16 + (lane >> 3) + (tile + first_tile) * LANES
        center = box * (leaf_count * box_ticks) + base
        offsets = (ticks - center).astype(jnp.float32).T
        for number, (cosine, sine) in enumerate(target_phases(offsets, group_cells, pair_count)):
            out_ref[tile, 2 * number] = cosine
            out_ref[tile, 2 * number + 1] = sine
        return carry

    lax.fori_loop(0, out_ref.shape[0], one_tile, 0, unroll=2)


def block_sums(phase_ref, roots, tile, rows, first):
    totals = [None, None]
    for node in range(HALF):
        for wave in range(2):
            phase = phase_ref[tile, 2 * node + wave, rows, :]
            for side in range(2):
                row = first + (2 * side + wave) * HALF + node
                term = phase * roots[pl.ds(row, 1), :]
                totals[side] = term if totals[side] is None else totals[side] + term
    return totals


def pair_field(phase_ref, root_refs, roots, sums, tile, column, pair, add_ref=None):
    low = lax.axis_index("blk") & 1
    for number, root_ref in enumerate(root_refs):
        rows = pl.ds((low ^ number) * ROWS, ROWS)
        roots[rows, :] = root_ref[:, pl.ds(pl.multiple_of(column, LANES), LANES)]
    plane = 2 * HALF + 2 + 2 * pair
    for first in range(0, TGT_BOX, ROW_CHUNK):
        rows = slice(first, first + ROW_CHUNK)
        high = block_sums(phase_ref, roots, tile, rows, ROWS)
        step = phase_ref[tile, 2 * HALF, rows, :], phase_ref[tile, 2 * HALF + 1, rows, :]
        real, imag = complex_product(step, high)
        low_real, low_imag = block_sums(phase_ref, roots, tile, rows, 0)
        start = phase_ref[tile, plane, rows, :], phase_ref[tile, plane + 1, rows, :]
        values = complex_product(start, (real + low_real, imag + low_imag))
        for side, value in enumerate(values):
            sums[side, rows, :] = value if add_ref is None else value + add_ref[side, rows, :]


def near_kernel(phase_ref, *refs, first_column):
    root_refs, (out_ref, roots) = refs[:2], refs[2:]
    pair = lax.axis_index("blk") >> 1

    def one_tile(tile, carry):
        column = (tile + first_column) * LANES
        pair_field(phase_ref, root_refs, roots, out_ref.at[tile], tile, column, pair)
        return carry

    lax.fori_loop(0, out_ref.shape[0], one_tile, 0)


def share_places(tile_counts):
    firsts = [sum(tile_counts[:part]) for part in range(len(tile_counts))]
    starts = {}
    for (_, chunk), first in zip(PHASE_SHARES, firsts):
        starts.setdefault(chunk, first)
    return firsts, [first - starts[chunk] for (_, chunk), first in zip(PHASE_SHARES, firsts)]


def far_kernel(*refs, masks):
    count = len(PHASE_SHARES)
    phase_refs, near_refs, root_refs = refs[:count], refs[count : 2 * count], refs[2 * count : -5]
    out_ref, roots, sums, rows_ref, semaphores = refs[-5:]
    firsts, places = share_places([near_ref.shape[0] for near_ref in near_refs])

    def out_copy(number):
        rows = pl.ds(pl.multiple_of(number * 2 * LANES, 2 * LANES), 2 * LANES)
        return pltpu.make_async_copy(
            rows_ref.at[number], out_ref.at[rows, :], semaphores.at[number]
        )

    def make(number, tile, part):
        chunk = PHASE_SHARES[part][1]
        column = (places[part] + tile) * LANES
        found = root_refs[chunk * len(masks) : (chunk + 1) * len(masks)]
        add_ref = near_refs[part].at[tile]
        for first in range(0, len(masks), 2):
            pair = (lax.axis_index("blk") ^ masks[first]) >> 1
            out = sums.at[number & 1]
            pair_roots = found[first : first + 2]
            pair_field(phase_refs[part], pair_roots, roots, out, tile, column, pair, add_ref)
            add_ref = out

    def put(number):
        for side in range(2):
            values = sums[number & 1, side].T
            for group in range(16):
                rows = pl.ds(2 * group + side, 8, stride=32)
                rows_ref[number, rows, :] = values[8 * group : 8 * group + 8]

    make(0, 0, 0)
    for part in range(count):

        def one_tile(tile, carry, part=part):
            number = firsts[part] + tile
            put(number - 1)
            make(number, tile, part)
            out_copy(number - 1).start()
            return carry

        lax.fori_loop(1 if part == 0 else 0, near_refs[part].shape[0], one_tile, 0)
    last = rows_ref.shape[0] - 1
    put(last)
    out_copy(last).start()
    for number in range(last + 1):
        out_copy(number).wait()


small_vmem = pltpu.CompilerParams(vmem_limit_bytes=6 * 2**20)


def in_vmem(value):
    return pltpu.with_memory_space_constraint(value, pltpu.VMEM)


def in_hbm(value):
    return pltpu.with_memory_space_constraint(value, pltpu.HBM)


def whole_vmem(count):
    return [pl.BlockSpec(memory_space=pltpu.VMEM)] * count


def partner_2(block, axis, apart):
    count = lax.axis_size(axis)
    route = []
    for low in range(count):
        high = low | 1 << apart
        if high != low and high < count:
            route += [(low, high), (high, low)]
    return lax.ppermute(block, axis, route)


def local(src_pos, strengths, tgt_pos):
    leaf_count = lax.axis_size("leaf")
    leaf_bits = leaf_count.bit_length() - 1
    box_count = src_pos.shape[1] // PER_BOX
    local_depth = box_count.bit_length() - 1
    assert box_count == 16 * LANES
    group_cells = box_count * leaf_count * BOX_CELLS
    box_ticks = TOP_TICKS // (box_count * leaf_count)
    offsets = node_offsets(group_cells)
    assert (offsets + offsets[::-1] == group_cells - 1).all()
    assert box_ticks // 2 * group_cells % 2**32 == 0

    tile_count = box_count // LANES
    part_tiles = [tile_count * share // 16 for share, _ in PHASE_SHARES]
    firsts, places = share_places(part_tiles)

    tables = source_tables() + [
        join_table(local_depth + bit_no, bit_no == leaf_bits - 1) for bit_no in range(leaf_bits)
    ]
    copied = [*tables, tgt_pos.reshape(box_count, TGT_BOX)]
    moments, *copied = pl.pallas_call(
        leaf_kernel,
        out_shape=[pltpu.VMEM((tile_count, ROWS, LANES), jnp.float32)]
        + [pltpu.VMEM(value.shape, value.dtype) for value in copied],
        in_specs=[pl.BlockSpec(memory_space=pl.ANY)] * (3 + len(copied)),
        out_specs=whole_vmem(1 + len(copied)),
        scratch_shapes=[
            pltpu.VMEM((box_count, PER_BOX), jnp.int32),
            pltpu.VMEM((2, box_count, PER_BOX), jnp.float32),
            pltpu.VMEM((16, BOX_CELLS), jnp.float32),
            pltpu.SemaphoreType.DMA((LEAF_STEPS,)),
            pltpu.SemaphoreType.DMA((LEAF_STEPS,)),
            pltpu.SemaphoreType.DMA,
            pltpu.SemaphoreType.DMA((len(copied),)),
        ],
        compiler_params=small_vmem,
        name="leaves",
    )(
        in_hbm(src_pos.reshape(box_count, PER_BOX)),
        in_hbm(strengths.reshape(2, box_count, PER_BOX)),
        in_hbm(cell_table()),
        *[in_hbm(value) for value in copied],
    )
    *tables, ticks = copied
    parts = pl.pallas_call(
        tree_kernel,
        out_shape=[pltpu.VMEM((ROWS, box_count // CHUNKS), jnp.float32)] * CHUNKS,
        in_specs=whole_vmem(5),
        out_specs=whole_vmem(CHUNKS),
        compiler_params=small_vmem,
        name="tree",
    )(in_vmem(moments), *[in_vmem(table) for table in tables[:-leaf_bits]])

    blk_count = lax.axis_size("blk")
    blk_bits = blk_count.bit_length() - 1
    plane_count = 2 * HALF + 2 + blk_count

    def make_phases(number, after):
        return pl.pallas_call(
            functools.partial(
                phase_kernel,
                first_tile=firsts[number],
                leaf_count=leaf_count,
                group_cells=group_cells,
                pair_count=blk_count // 2,
            ),
            out_shape=pltpu.VMEM((part_tiles[number], plane_count, TGT_BOX, LANES), jnp.float32),
            in_specs=whole_vmem(1) + [pl.BlockSpec(memory_space=pl.ANY)],
            out_specs=pl.BlockSpec(memory_space=pltpu.VMEM),
            compiler_params=small_vmem,
            name="phases",
        )(in_vmem(ticks), after)

    def join(part, partner, bit_no):
        return pl.pallas_call(
            functools.partial(join_kernel, bit_no=bit_no),
            out_shape=pltpu.VMEM(part.shape, jnp.float32),
            in_specs=whole_vmem(3),
            out_specs=pl.BlockSpec(memory_space=pltpu.VMEM),
            compiler_params=small_vmem,
            name="join",
        )(in_vmem(part), in_vmem(partner), in_vmem(tables[bit_no - leaf_bits]))

    def near_field(number, roots):
        return pl.pallas_call(
            functools.partial(near_kernel, first_column=places[number]),
            out_shape=pltpu.VMEM((part_tiles[number], 2, TGT_BOX, LANES), jnp.float32),
            in_specs=whole_vmem(3),
            out_specs=pl.BlockSpec(memory_space=pltpu.VMEM),
            scratch_shapes=[pltpu.VMEM((2 * ROWS, LANES), jnp.float32)],
            compiler_params=small_vmem,
            name="near",
        )(in_vmem(phases[number]), *[in_vmem(root) for root in roots])

    phases = []
    for bit_no in range(leaf_bits):
        stage = "last" if bit_no == leaf_bits - 1 else f"bit_{bit_no}"
        partners = []
        for part in parts:
            partners.append(partner_2(part, "leaf", bit_no))
        for number in PHASE_PLAN.get(stage, ()):
            phases.append(make_phases(number, parts[0]))
            partners[0], phases[-1] = lax.optimization_barrier((partners[0], phases[-1]))
        joined = []
        for part, partner in zip(parts, partners):
            joined.append(join(part, partner, bit_no))
        parts = joined
    masks = list(range(2, blk_count))
    founds = []
    for part in parts:
        found = {0: part, 1: partner_2(part, "blk", 0)}
        for blk_bit in range(1, blk_bits):
            found[1 << blk_bit] = partner_2(part, "blk", blk_bit)
        founds.append(found)
    near = []
    for number, (_, chunk) in enumerate(PHASE_SHARES):
        near.append(near_field(number, (founds[chunk][0], founds[chunk][1])))
    founds[0][2], *near[:3] = lax.optimization_barrier((founds[0][2], *near[:3]))
    founds[1][2], near[3] = lax.optimization_barrier((founds[1][2], near[3]))
    for found in founds:
        for mask in masks:
            if mask not in found:
                low_bit = mask & -mask
                found[mask] = partner_2(
                    found[mask ^ low_bit], "blk", low_bit.bit_length() - 1
                )
    operands = [*phases, *near, *[found[mask] for found in founds for mask in masks]]
    field = pl.pallas_call(
        functools.partial(far_kernel, masks=masks),
        out_shape=jax.ShapeDtypeStruct((2 * box_count, TGT_BOX), jnp.float32),
        in_specs=whole_vmem(len(operands)),
        out_specs=pl.BlockSpec(memory_space=pl.ANY),
        scratch_shapes=[
            pltpu.VMEM((2 * ROWS, LANES), jnp.float32),
            pltpu.VMEM((2, 2, TGT_BOX, LANES), jnp.float32),
            pltpu.VMEM((tile_count, 2 * LANES, TGT_BOX), jnp.float32),
            pltpu.SemaphoreType.DMA((tile_count,)),
        ],
        compiler_params=small_vmem,
        name="far",
    )(*[in_vmem(value) for value in operands])
    field = field.reshape(box_count, 2, TGT_BOX)
    return jnp.transpose(field, (1, 0, 2)).reshape(2, box_count * TGT_BOX)


def solution(mesh):
    return jax.shard_map(
        local,
        mesh=mesh,
        in_specs=(P("blk", "leaf"), P(None, "blk", "leaf"), P(("leaf", "blk"))),
        out_specs=P(None, ("leaf", "blk")),
        check_vma=False,
    )
```

```python
import functools

import jax
import jax.numpy as jnp
import numpy as np
from jax import lax
from jax.experimental import pallas as pl
from jax.experimental.pallas import tpu as pltpu
from jax.sharding import PartitionSpec as P


R = 16
PER_BOX = 128
TGT_BOX = 128
BOX_CELLS = 128
TOP_TICKS = 201326592
LANES = 128
ROWS = 2 * R
HALF = R // 2
CHUNKS = 2
PHASE_SHARES = ((6, 0), (2, 0), (4, 1), (2, 1), (2, 1))
PHASE_PLAN = {"bit_0": (0,), "bit_1": (1,), "last": (2, 3, 4)}
LEAF_STEPS = 4
LEAF_AHEAD = 2
ROW_CHUNK = 64

SIN_COEFS = (4.44288292, -7.30824569, 3.60635422, -0.84611165, 0.10982452)
COS_COEFS = (1.4142135, -6.97885095, 5.73946038, -1.88355791, 0.31068803)


def node_offsets(box_cells):
    node_index = np.arange(R)
    unit_nodes = (1.0 - np.cos(np.pi * (node_index + 0.5) / R)) / 2.0
    return np.floor(box_cells * unit_nodes).astype(np.int64)


def lagrange_values(node_pos, points):
    basis_rows = []
    for row_node in range(node_pos.shape[0]):
        column = np.ones(points.shape[0])
        for other_node in range(node_pos.shape[0]):
            if other_node != row_node:
                column = (
                    column
                    * (points - node_pos[other_node])
                    / (node_pos[row_node] - node_pos[other_node])
                )
        basis_rows.append(column)
    return np.stack(basis_rows)


def turn_exp(ticks, cells):
    product = (ticks * cells) % 2**32
    return np.exp(2j * np.pi * (product / 2.0**32))


def as_real(matrix):
    return np.block([[matrix.real, -matrix.imag], [matrix.imag, matrix.real]])


def level_blocks(tree_level):
    child_cells = BOX_CELLS * 2**tree_level
    box_ticks = TOP_TICKS // 2**tree_level
    assert box_ticks // 2 * child_cells % 2**32 == 0
    child_nodes = node_offsets(child_cells)
    parent_nodes = node_offsets(2 * child_cells)
    inner_cells = np.concatenate([child_nodes, child_nodes + child_cells])
    blend = lagrange_values(
        parent_nodes / (2.0 * child_cells), inner_cells / (2.0 * child_cells)
    ).reshape(R, 2, R)
    blend = blend.astype(np.float32).astype(np.float64)
    center = box_ticks // 4
    return [
        [
            blend[:, child]
            * turn_exp((2 * half - 1) * (box_ticks // 4), child_nodes)[None, :]
            * turn_exp(center, child * child_cells)
            for child in range(2)
        ]
        for half in range(2)
    ]


def stage_matrix(first_level, order):
    count = len(order)
    size = 2**count
    levels = [level_blocks(first_level + step) for step in range(count)]
    place = [order.index(step) for step in range(count)]
    full = np.zeros((size, ROWS, size, ROWS))
    for out_block in range(size):
        for in_block in range(size):
            matrix = np.eye(R)
            for step in range(count):
                bits = (out_block >> place[step] & 1, in_block >> place[step] & 1)
                matrix = levels[step][bits[0]][bits[1]] @ matrix
            full[out_block, :, in_block, :] = as_real(matrix)
    return full


def product_basis():
    table = np.zeros((R, R))
    for high in range(4):
        for low in range(4):
            for degree in (4 * high + low, abs(4 * high - low)):
                table[4 * high + low, degree] += 0.5
    return table


def leaf_matrix():
    leaf_nodes = node_offsets(BOX_CELLS)
    node_angles = np.pi * (np.arange(R) + 0.5) / R
    at_exact = lagrange_values(2.0 * leaf_nodes / BOX_CELLS - 1.0, np.cos(node_angles))
    cheb_at = np.stack([np.cos(degree * node_angles) for degree in range(R)])
    norm_weights = np.where(np.arange(R) == 0, 1.0, 2.0) / R
    coefficients = norm_weights[:, None] * (cheb_at @ at_exact.T)
    coefficients = coefficients.astype(np.float32).astype(np.float64)
    return as_real(coefficients.T @ np.linalg.inv(product_basis()))


def field_rows():
    table = np.zeros((4, HALF, 2, R))
    for node in range(HALF):
        mirror = R - 1 - node
        table[0, node, 0, [node, mirror]] = 1.0
        table[1, node, 1, [node, mirror]] = [1.0, -1.0]
        table[2, node, 1, [node, mirror]] = 1.0
        table[3, node, 0, [node, mirror]] = [-1.0, 1.0]
    return table.reshape(ROWS, ROWS)


def split_table(matrix):
    high = matrix.astype(np.float32).astype(jnp.bfloat16)
    low = (matrix - high.astype(np.float64)).astype(np.float32).astype(jnp.bfloat16)
    return np.concatenate([high, high, low], axis=-1)


def split_value(value):
    high = value.astype(jnp.bfloat16)
    low = (value - high.astype(jnp.float32)).astype(jnp.bfloat16)
    return jnp.concatenate([high, low, high], axis=0)


def times_table(table, value):
    return jnp.dot(table, split_value(value), preferred_element_type=jnp.float32)


def polynomial(coefs, value):
    total = jnp.full_like(value, coefs[-1])
    for coef in coefs[-2::-1]:
        total = total * value + coef
    return total


def unit_circle(turns):
    rest = turns - jnp.round(turns)
    square = rest * rest
    sine = rest * polynomial(SIN_COEFS, square)
    cosine = polynomial(COS_COEFS, square)
    return 1.0 - sine * sine, sine * cosine


def reverse_bits(value, count):
    return sum((value >> bit & 1) << (count - 1 - bit) for bit in range(count))


def swap_bits(blocks, block_bit, lane_bit):
    lane = lax.broadcasted_iota(jnp.int32, (8, LANES), 1)
    upper = (lax.broadcasted_iota(jnp.int32, blocks[0].shape, 1) >> lane_bit & 1) == 1
    swapped = list(blocks)
    for number in range(len(blocks)):
        if not number >> block_bit & 1:
            other = number | 1 << block_bit
            low, high = blocks[number], blocks[other]
            mixed = jnp.where(upper, low, high)
            moved = jnp.concatenate(
                [pick_lanes(mixed[row : row + 8], lane ^ 1 << lane_bit) for row in range(0, ROWS, 8)],
                axis=0,
            )
            swapped[number] = jnp.where(upper, moved, low)
            swapped[other] = jnp.where(upper, high, moved)
    return swapped


def run_stage(blocks, row_bits, table):
    count = len(blocks)
    side_bits = [bit for bit in range(count.bit_length() - 1) if bit not in row_bits]

    def number(row, side):
        return sum((row >> k & 1) << bit for k, bit in enumerate(row_bits)) + sum(
            (side >> k & 1) << bit for k, bit in enumerate(side_bits)
        )

    sides = range(2 ** len(side_bits))
    rows = range(2 ** len(row_bits))
    value = jnp.concatenate(
        [
            jnp.concatenate([blocks[number(row, side)] for row in rows], axis=0)
            for side in sides
        ],
        axis=1,
    )
    product = times_table(table, value)
    result = list(blocks)
    for side in sides:
        for row in rows:
            result[number(row, side)] = product[
                row * ROWS : (row + 1) * ROWS, side * LANES : (side + 1) * LANES
            ]
    return result


def cell_table():
    turned = turn_exp(TOP_TICKS // 2, np.arange(BOX_CELLS))
    return jnp.asarray(np.repeat([turned.real, turned.imag], 8, axis=0), jnp.float32)


def pick_lanes(table, lanes):
    numbers = lax.GatherDimensionNumbers(
        offset_dims=(),
        collapsed_slice_dims=(1,),
        start_index_map=(1,),
        operand_batching_dims=(0,),
        start_indices_batching_dims=(0,),
    )
    return lax.gather(
        table, lanes[..., None], numbers, (1, 1), mode=lax.GatherScatterMode.PROMISE_IN_BOUNDS
    )


def sublane_sums(values):
    sublane = lax.broadcasted_iota(jnp.int32, (8, LANES), 0)
    for step in (4, 2, 1):
        lower = (sublane & step) == 0
        values = [
            jnp.where(lower, first, second)
            + pltpu.roll(jnp.where(lower, second, first), step, 0)
            if step == 4
            else jnp.where(lower, first, second)
            + jnp.where(lower, pltpu.roll(first, 8 - step, 0), pltpu.roll(second, step, 0))
            for first, second in zip(values[:step], values[step:])
        ]
    return values[0]


def leaf_kernel(pos_hbm, strength_hbm, table_hbm, *refs):
    count = (len(refs) - 8) // 2
    out_ref, pos_ref, strength_ref, table_ref = refs[count], *refs[2 * count + 1 : 2 * count + 4]
    pos_done, strength_done, table_done, other_done = refs[2 * count + 4 :]
    others = [
        pltpu.make_async_copy(source, target, other_done.at[number])
        for number, (source, target) in enumerate(zip(refs[:count], refs[count + 1 :]))
    ]
    table_copy = pltpu.make_async_copy(table_hbm, table_ref, table_done)
    size = pos_ref.shape[0] // LEAF_STEPS

    def step_copies(step):
        rows = pl.ds(pl.multiple_of(step * size, LANES), size)
        yield pltpu.make_async_copy(pos_hbm.at[rows, :], pos_ref.at[rows, :], pos_done.at[step])
        yield pltpu.make_async_copy(
            strength_hbm.at[:, rows, :], strength_ref.at[:, rows, :], strength_done.at[step]
        )

    table_copy.start()
    for step in range(LEAF_AHEAD):
        for copy in step_copies(step):
            copy.start()

    def one_tile(tile):
        parts = [[], [], []]
        for group in range(16):
            start = tile * LANES + 8 * reverse_bits(group, 4)
            rows = pl.ds(pl.multiple_of(start, 8), 8)
            parts[0].append(pos_ref[rows, :] & (BOX_CELLS - 1))
            parts[1].append(strength_ref[0, rows, :])
            parts[2].append(strength_ref[1, rows, :])
        cells, real, imag = (jnp.concatenate(part, axis=0).T for part in parts)
        sums = [None] * ROWS
        for group in range(16):
            rows = slice(8 * group, 8 * group + 8)
            turn = [pick_lanes(table_ref[8 * row : 8 * row + 8, :], cells[rows]) for row in range(2)]
            turned = complex_product(turn, (real[rows], imag[rows]))
            v = cells[rows].astype(jnp.float32) * (2.0 / BOX_CELLS) - 1.0
            t2 = 2.0 * (v * v) - 1.0
            t3 = v * (2.0 * t2 - 1.0)
            t4 = 2.0 * (t2 * t2) - 1.0
            t8 = 2.0 * (t4 * t4) - 1.0
            t12 = t4 * (2.0 * t8 - 1.0)
            for side, value in enumerate(turned):
                for high, outer in enumerate((None, t4, t8, t12)):
                    base = value if outer is None else value * outer
                    for low, inner in enumerate((None, v, t2, t3)):
                        term = base if inner is None else base * inner
                        row = side * R + 4 * high + low
                        sums[row] = term if sums[row] is None else sums[row] + term
        for row in range(0, ROWS, 8):
            out_ref[tile, pl.ds(row, 8), :] = sublane_sums(sums[row : row + 8])

    def one_step(step, carry):
        for copy in step_copies(step):
            copy.wait()

        @pl.when(step < LEAF_STEPS - LEAF_AHEAD)
        def start_later():
            for copy in step_copies(step + LEAF_AHEAD):
                copy.start()

        @pl.when(step == LEAF_STEPS - LEAF_AHEAD)
        def start_others():
            for copy in others:
                copy.start()

        for tile in range(size // LANES):
            one_tile(step * (size // LANES) + tile)
        return carry

    table_copy.wait()
    lax.fori_loop(0, LEAF_STEPS, one_step, 0)
    for copy in others:
        copy.wait()


def tree_kernel(moment_ref, t1_ref, t2_ref, t3_ref, t4_ref, *out_refs):
    tile_count = moment_ref.shape[0]
    blocks = [moment_ref[tile] for tile in range(tile_count)]
    for block_bit, lane_bit in ((0, 2), (1, 1), (2, 0)):
        blocks = swap_bits(blocks, block_bit, lane_bit)
    blocks = run_stage(blocks, (0, 1, 2), t1_ref[...])
    for block_bit, lane_bit in ((2, 6), (1, 5), (0, 4)):
        blocks = swap_bits(blocks, block_bit, lane_bit)
    blocks = run_stage(blocks, (0, 1, 2), t2_ref[...])
    for block_bit, lane_bit in ((2, 3), (1, 2), (0, 1)):
        blocks = swap_bits(blocks, block_bit, lane_bit)
    blocks = run_stage(blocks, (0, 1, 2), t3_ref[...])
    blocks = swap_bits(blocks, 2, 0)
    blocks = run_stage(blocks, (2, 3), t4_ref[...])
    for block_bit, lane_bit in ((3, 3), (2, 4), (0, 5), (1, 6)):
        blocks = swap_bits(blocks, block_bit, lane_bit)
    for number in range(tile_count):
        place = sum((number >> bit & 1) << to for bit, to in ((1, 3), (0, 2), (2, 1), (3, 0)))
        part, column = divmod(place, tile_count // len(out_refs))
        out_refs[part][:, column * LANES : (column + 1) * LANES] = blocks[number]


def source_tables():
    first = stage_matrix(0, [2, 1, 0])
    first = np.einsum("abcd,de->abce", first, leaf_matrix())
    second = stage_matrix(3, [2, 1, 0])
    third = stage_matrix(6, [2, 1, 0])
    fourth = stage_matrix(9, [0, 1])
    return [
        jnp.asarray(split_table(table.reshape(len(table) * ROWS, -1)))
        for table in (first, second, third, fourth)
    ]


def join_kernel(own_ref, partner_ref, table_ref, out_ref, *, bit_no):
    side = lax.axis_index("leaf") >> bit_no & 1
    value = jnp.concatenate([own_ref[...], partner_ref[...]], axis=0)
    out_ref[...] = times_table(table_ref[side], value)


def join_table(tree_level, last):
    blocks = level_blocks(tree_level)
    sides = []
    for side in range(2):
        table = np.concatenate(
            [as_real(blocks[side][side]), as_real(blocks[side][1 - side])], axis=1
        )
        sides.append(split_table(field_rows() @ table if last else table))
    return jnp.asarray(np.stack(sides))


def box_rows(first):
    return pl.ds(first, 8, stride=16)


def complex_product(left, right):
    return left[0] * right[0] - left[1] * right[1], left[0] * right[1] + left[1] * right[0]


def square_of(value):
    double = 2.0 * value[1]
    return 1.0 - double * value[1], double * value[0]


def target_phases(offsets, group_cells, pair_count):
    rates = (group_cells - 1 - 2 * node_offsets(group_cells)[:HALF]) / 2.0**33
    found = [unit_circle(offsets * float(rate)) for rate in rates]
    middle = unit_circle(offsets * float((group_cells - 1) / 2.0**33))
    step = unit_circle(offsets * float(group_cells / 2.0**32))
    twice = square_of(step)
    found += [step, middle]
    for _ in range(1, pair_count):
        found.append(complex_product(found[-1], twice))
    return found


def phase_kernel(tgt_ref, after_ref, out_ref, *, first_tile, leaf_count, group_cells, pair_count):
    box_ticks = TOP_TICKS // (group_cells // BOX_CELLS)
    leaf_no = lax.axis_index("leaf")
    leaf_bits = leaf_count.bit_length() - 1
    low_box = sum((leaf_no >> bit & 1) << (leaf_bits - 1 - bit) for bit in range(leaf_bits))
    base = low_box * box_ticks + box_ticks // 2

    def one_tile(tile, carry):
        ticks = [tgt_ref[box_rows((tile + first_tile) * LANES + group), :] for group in range(16)]
        ticks = jnp.concatenate(ticks, axis=0)
        lane = lax.broadcasted_iota(jnp.int32, ticks.shape, 0)
        box = (lane & 7) * 16 + (lane >> 3) + (tile + first_tile) * LANES
        center = box * (leaf_count * box_ticks) + base
        offsets = (ticks - center).astype(jnp.float32).T
        for number, (cosine, sine) in enumerate(target_phases(offsets, group_cells, pair_count)):
            out_ref[tile, 2 * number] = cosine
            out_ref[tile, 2 * number + 1] = sine
        return carry

    lax.fori_loop(0, out_ref.shape[0], one_tile, 0, unroll=2)


def block_sums(phase_ref, roots, tile, rows, first):
    totals = [None, None]
    for node in range(HALF):
        for wave in range(2):
            phase = phase_ref[tile, 2 * node + wave, rows, :]
            for side in range(2):
                row = first + (2 * side + wave) * HALF + node
                term = phase * roots[pl.ds(row, 1), :]
                totals[side] = term if totals[side] is None else totals[side] + term
    return totals


def pair_field(phase_ref, root_refs, roots, sums, tile, column, pair, add_ref=None):
    low = lax.axis_index("blk") & 1
    for number, root_ref in enumerate(root_refs):
        rows = pl.ds((low ^ number) * ROWS, ROWS)
        roots[rows, :] = root_ref[:, pl.ds(pl.multiple_of(column, LANES), LANES)]
    plane = 2 * HALF + 2 + 2 * pair
    for first in range(0, TGT_BOX, ROW_CHUNK):
        rows = slice(first, first + ROW_CHUNK)
        high = block_sums(phase_ref, roots, tile, rows, ROWS)
        step = phase_ref[tile, 2 * HALF, rows, :], phase_ref[tile, 2 * HALF + 1, rows, :]
        real, imag = complex_product(step, high)
        low_real, low_imag = block_sums(phase_ref, roots, tile, rows, 0)
        start = phase_ref[tile, plane, rows, :], phase_ref[tile, plane + 1, rows, :]
        values = complex_product(start, (real + low_real, imag + low_imag))
        for side, value in enumerate(values):
            sums[side, rows, :] = value if add_ref is None else value + add_ref[side, rows, :]


def near_kernel(phase_ref, *refs, first_column):
    root_refs, (out_ref, roots) = refs[:2], refs[2:]
    pair = lax.axis_index("blk") >> 1

    def one_tile(tile, carry):
        column = (tile + first_column) * LANES
        pair_field(phase_ref, root_refs, roots, out_ref.at[tile], tile, column, pair)
        return carry

    lax.fori_loop(0, out_ref.shape[0], one_tile, 0, unroll=True)


def share_places(tile_counts):
    firsts = [sum(tile_counts[:part]) for part in range(len(tile_counts))]
    starts = {}
    for (_, chunk), first in zip(PHASE_SHARES, firsts):
        starts.setdefault(chunk, first)
    return firsts, [first - starts[chunk] for (_, chunk), first in zip(PHASE_SHARES, firsts)]


def far_kernel(*refs, masks, parts, firsts, places, early_firsts=None):
    count = len(parts)
    phase_refs, near_refs, refs = refs[:count], refs[count : 2 * count], refs[2 * count :]
    root_refs, refs = refs[: len(masks)], refs[len(masks) :]
    final = early_firsts is not None
    if final:
        early_refs, (out_ref, roots, sums, rows_ref, semaphores) = refs[:-5], refs[-5:]
    else:
        rows_ref, roots, sums = refs
    sizes = [near_ref.shape[0] for near_ref in near_refs]
    tile_rows = 2 * LANES
    copies = []

    def out_copy(source, first, size, semaphore):
        rows = pl.ds(pl.multiple_of(first * tile_rows, tile_rows), size)
        return pltpu.make_async_copy(source, out_ref.at[rows, :], semaphore)

    def tile_copy(number):
        rows = pl.ds(pl.multiple_of(number * tile_rows, tile_rows), tile_rows)
        first = firsts[parts[0]] + number
        return out_copy(rows_ref.at[rows, :], first, tile_rows, semaphores.at[number])

    if final:
        for number, (early_ref, first) in enumerate(zip(early_refs, early_firsts)):
            semaphore = semaphores.at[sum(sizes) + number]
            copies.append(out_copy(early_ref, first, early_ref.shape[0], semaphore))
            copies[-1].start()

    def make(number, tile, part):
        column = (places[parts[part]] + tile) * LANES
        add_ref = near_refs[part].at[tile]
        for first in range(0, len(masks), 2):
            pair = (lax.axis_index("blk") ^ masks[first]) >> 1
            out = sums.at[number & 1]
            pair_roots = root_refs[first : first + 2]
            pair_field(phase_refs[part], pair_roots, roots, out, tile, column, pair, add_ref)
            add_ref = out

    def put(number):
        for side in range(2):
            values = sums[number & 1, side].T
            for group in range(16):
                rows = pl.ds(number * tile_rows + 2 * group + side, 8, stride=32)
                rows_ref[rows, :] = values[8 * group : 8 * group + 8]

    make(0, 0, 0)
    for part in range(count):

        def one_tile(tile, carry, part=part):
            number = sum(sizes[:part]) + tile
            put(number - 1)
            make(number, tile, part)
            if final:
                tile_copy(number - 1).start()
            return carry

        lax.fori_loop(1 if part == 0 else 0, sizes[part], one_tile, 0)
    last = sum(sizes) - 1
    put(last)
    if final:
        tile_copy(last).start()
        for number in range(last + 1):
            tile_copy(number).wait()
        for copy in copies:
            copy.wait()


small_vmem = pltpu.CompilerParams(vmem_limit_bytes=6 * 2**20)


def in_vmem(value):
    return pltpu.with_memory_space_constraint(value, pltpu.VMEM)


def in_hbm(value):
    return pltpu.with_memory_space_constraint(value, pltpu.HBM)


def whole_vmem(count):
    return [pl.BlockSpec(memory_space=pltpu.VMEM)] * count


def partner_2(block, axis, apart):
    count = lax.axis_size(axis)
    route = []
    for low in range(count):
        high = low | 1 << apart
        if high != low and high < count:
            route += [(low, high), (high, low)]
    return lax.ppermute(block, axis, route)


def local(src_pos, strengths, tgt_pos):
    leaf_count = lax.axis_size("leaf")
    leaf_bits = leaf_count.bit_length() - 1
    box_count = src_pos.shape[1] // PER_BOX
    local_depth = box_count.bit_length() - 1
    assert box_count == 16 * LANES
    group_cells = box_count * leaf_count * BOX_CELLS
    box_ticks = TOP_TICKS // (box_count * leaf_count)
    offsets = node_offsets(group_cells)
    assert (offsets + offsets[::-1] == group_cells - 1).all()
    assert box_ticks // 2 * group_cells % 2**32 == 0

    tile_count = box_count // LANES
    part_tiles = [tile_count * share // 16 for share, _ in PHASE_SHARES]
    firsts, places = share_places(part_tiles)

    tables = source_tables() + [
        join_table(local_depth + bit_no, bit_no == leaf_bits - 1) for bit_no in range(leaf_bits)
    ]
    copied = [*tables, tgt_pos.reshape(box_count, TGT_BOX)]
    moments, *copied = pl.pallas_call(
        leaf_kernel,
        out_shape=[pltpu.VMEM((tile_count, ROWS, LANES), jnp.float32)]
        + [pltpu.VMEM(value.shape, value.dtype) for value in copied],
        in_specs=[pl.BlockSpec(memory_space=pl.ANY)] * (3 + len(copied)),
        out_specs=whole_vmem(1 + len(copied)),
        scratch_shapes=[
            pltpu.VMEM((box_count, PER_BOX), jnp.int32),
            pltpu.VMEM((2, box_count, PER_BOX), jnp.float32),
            pltpu.VMEM((16, BOX_CELLS), jnp.float32),
            pltpu.SemaphoreType.DMA((LEAF_STEPS,)),
            pltpu.SemaphoreType.DMA((LEAF_STEPS,)),
            pltpu.SemaphoreType.DMA,
            pltpu.SemaphoreType.DMA((len(copied),)),
        ],
        compiler_params=small_vmem,
        name="leaves",
    )(
        in_hbm(src_pos.reshape(box_count, PER_BOX)),
        in_hbm(strengths.reshape(2, box_count, PER_BOX)),
        in_hbm(cell_table()),
        *[in_hbm(value) for value in copied],
    )
    *tables, ticks = copied
    parts = pl.pallas_call(
        tree_kernel,
        out_shape=[pltpu.VMEM((ROWS, box_count // CHUNKS), jnp.float32)] * CHUNKS,
        in_specs=whole_vmem(5),
        out_specs=whole_vmem(CHUNKS),
        compiler_params=small_vmem,
        name="tree",
    )(in_vmem(moments), *[in_vmem(table) for table in tables[:-leaf_bits]])

    blk_count = lax.axis_size("blk")
    blk_bits = blk_count.bit_length() - 1
    plane_count = 2 * HALF + 2 + blk_count

    def make_phases(number, after):
        return pl.pallas_call(
            functools.partial(
                phase_kernel,
                first_tile=firsts[number],
                leaf_count=leaf_count,
                group_cells=group_cells,
                pair_count=blk_count // 2,
            ),
            out_shape=pltpu.VMEM((part_tiles[number], plane_count, TGT_BOX, LANES), jnp.float32),
            in_specs=whole_vmem(1) + [pl.BlockSpec(memory_space=pl.ANY)],
            out_specs=pl.BlockSpec(memory_space=pltpu.VMEM),
            compiler_params=small_vmem,
            name="phases",
        )(in_vmem(ticks), after)

    def join(part, partner, bit_no):
        return pl.pallas_call(
            functools.partial(join_kernel, bit_no=bit_no),
            out_shape=pltpu.VMEM(part.shape, jnp.float32),
            in_specs=whole_vmem(3),
            out_specs=pl.BlockSpec(memory_space=pltpu.VMEM),
            compiler_params=small_vmem,
            name="join",
        )(in_vmem(part), in_vmem(partner), in_vmem(tables[bit_no - leaf_bits]))

    def near_field(number, roots):
        return pl.pallas_call(
            functools.partial(near_kernel, first_column=places[number]),
            out_shape=pltpu.VMEM((part_tiles[number], 2, TGT_BOX, LANES), jnp.float32),
            in_specs=whole_vmem(3),
            out_specs=pl.BlockSpec(memory_space=pltpu.VMEM),
            scratch_shapes=[pltpu.VMEM((2 * ROWS, LANES), jnp.float32)],
            compiler_params=small_vmem,
            name="near",
        )(in_vmem(phases[number]), *[in_vmem(root) for root in roots])

    phases = []
    for bit_no in range(leaf_bits):
        stage = "last" if bit_no == leaf_bits - 1 else f"bit_{bit_no}"
        partners = []
        for part in parts:
            partners.append(partner_2(part, "leaf", bit_no))
        for number in PHASE_PLAN.get(stage, ()):
            phases.append(make_phases(number, parts[0]))
            partners[0], phases[-1] = lax.optimization_barrier((partners[0], phases[-1]))
        joined = []
        for part, partner in zip(parts, partners):
            joined.append(join(part, partner, bit_no))
        parts = joined
    masks = list(range(2, blk_count))
    founds = []
    for part in parts:
        found = {0: part, 1: partner_2(part, "blk", 0)}
        for blk_bit in range(1, blk_bits):
            found[1 << blk_bit] = partner_2(part, "blk", blk_bit)
        founds.append(found)
    near = []
    for number, (_, chunk) in enumerate(PHASE_SHARES):
        near.append(near_field(number, (founds[chunk][0], founds[chunk][1])))

    def forward(chunk):
        found = founds[chunk]
        for mask in masks:
            if mask not in found:
                low_bit = mask & -mask
                found[mask] = partner_2(
                    found[mask ^ low_bit], "blk", low_bit.bit_length() - 1
                )

    def far_field(chunk, parts, early=None):
        operands = [phases[part] for part in parts] + [near[part] for part in parts]
        operands += [founds[chunk][mask] for mask in masks]
        tiles = sum(part_tiles[part] for part in parts)
        rows = pltpu.VMEM((2 * tiles * LANES, TGT_BOX), jnp.float32)
        settings = dict(masks=masks, parts=parts, firsts=firsts, places=places)
        scratch = [
            pltpu.VMEM((2 * ROWS, LANES), jnp.float32),
            pltpu.VMEM((2, 2, TGT_BOX, LANES), jnp.float32),
        ]
        if early:
            operands += early.values()
            settings["early_firsts"] = [firsts[part] for part in early]
            scratch += [rows, pltpu.SemaphoreType.DMA((tiles + len(early),))]
        return pl.pallas_call(
            functools.partial(far_kernel, **settings),
            out_shape=jax.ShapeDtypeStruct((2 * box_count, TGT_BOX), jnp.float32)
            if early
            else rows,
            in_specs=whole_vmem(len(operands)),
            out_specs=pl.BlockSpec(memory_space=pl.ANY if early else pltpu.VMEM),
            scratch_shapes=scratch,
            compiler_params=small_vmem,
            name="far",
        )(*[in_vmem(value) for value in operands])

    founds[0][2], *near[:3] = lax.optimization_barrier((founds[0][2], *near[:3]))
    forward(0)
    early = {}
    early[1] = far_field(0, (1,))
    founds[1][2], near[3], near[4], early[1] = lax.optimization_barrier(
        (founds[1][2], near[3], near[4], early[1])
    )
    forward(1)
    early[0] = far_field(0, (0,))
    field = far_field(1, (2, 3, 4), early)
    field = field.reshape(box_count, 2, TGT_BOX)
    return jnp.transpose(field, (1, 0, 2)).reshape(2, box_count * TGT_BOX)


def solution(mesh):
    return jax.shard_map(
        local,
        mesh=mesh,
        in_specs=(P("blk", "leaf"), P(None, "blk", "leaf"), P(("leaf", "blk"))),
        out_specs=P(None, ("leaf", "blk")),
        check_vma=False,
    )
```
